512 devices in a mesh: groups: 2 (over y), blk: 32 (over z), head: 4 (over x), pair: 2 (over core).
Axes of the slice: x: 4, y: 2, z: 32, core: 2. Of those that a mesh axis runs over, the one named last changes fastest.
The devices are a block of a 4x8x32 slice.
Arguments:
- single: bfloat16 [2048, 384], P(('groups', 'blk')), parts along dimension 0, may hold values from -6 to 6
- pair: bfloat16 [2048, 32, 32, 128], P(('groups', 'blk'), None, 'pair'), parts along dimension 0, may hold values from -6 to 6
- frames: float32 [12, 2048], P(None, ('groups', 'blk')), parts along dimension 1, as said below
- chain: int32 [2048], P(('groups', 'blk')), parts along dimension 0, may hold values from 0 to 5, never falling along the last dimension, each value on 1 to 341 neighbouring positions
- mask: int32 [2048], P(('groups', 'blk')), parts along dimension 0, may hold values 0 or 1
- w_query: bfloat16 [384, 192], P(None, 'head'), may hold values from -0.3125 to 0.3125
- w_key_value: bfloat16 [384, 384], P(None, 'head'), may hold values from -0.3125 to 0.3125
- w_query_points: bfloat16 [384, 144], P(None, 'head'), may hold values from -0.3125 to 0.3125
- w_kv_points: bfloat16 [384, 432], P(None, 'head'), may hold values from -0.3125 to 0.3125
- w_pair_bias: bfloat16 [128, 12], P(None, 'head'), may hold values from -0.5 to 0.5
- head_weights: float32 [12], P('head'), may hold values from -9 to 1
- chain_bias: float32 [12], P('head'), may hold values from -3 to 3
- w_out: bfloat16 [12, 176, 384], P('head'), may hold values from -0.125 to 0.125
- out_gain: float32 [384], replicated, may hold values from 0.5 to 1.5
- w_backbone: bfloat16 [384, 6], replicated, may hold values from -0.3125 to 0.3125
Outputs:
- single_out: bfloat16 [2048, 384], P(('groups', 'blk')), parts along dimension 0
- frames_out: float32 [12, 2048], P(None, 'groups'), parts along dimension 1
The draws below stay inside these ranges and needn't reach their ends.
There are 2 independent parts, one for each index of `groups`. The reference program is written for one: setup_inputs(seed, part) draws one part's arguments, and reference() takes and returns one part's arrays. A program takes and returns all parts, laid end to end along the dimension named above; an argument that names none is the same for every part. Nothing has to cross between parts.
Inputs may be any that keep to these rules, and one draw needn't show every extreme that they name: `frames`: rows 0 to 8 of every column hold an orthonormal rotation matrix row by row; rows 9 to 11 the translation.
All inputs are finite; a program needn't handle non-finite values. No bound on the sum of `mask` on one device may be relied on, other than what follows from the above.
Results may differ from the reference program's by a relative error of at most 0.0048.
Values sent between devices are 32-bit elements; how exact they have to be, the bound alone decides.
No kernel may reach another device: no remote copies, remote signals or barrier semaphores. Data moves between devices by JAX's collectives and lax.ppermute only.
A program may use at most 64 MiB of HBM per device.

```python
import math
import jax
import jax.numpy as jnp
import numpy as np
from jax import lax

C = 384
CZ = 128
HEADS = 12
CH = 16
PQ = 4
PV = 8
ROW_DEV = 32
N_RES = 1024
KEY_BLOCKS = 32
CAT = 176
N_BLK = 32


def draw_frames(key, part):
    key_turn = jax.random.fold_in(key, 101)
    key_walk = jax.random.fold_in(key, 202)
    quaternion = jax.random.normal(key_turn, (4, N_RES), jnp.float32)
    quaternion = quaternion / jnp.sqrt(jnp.sum(quaternion * quaternion, axis=0, keepdims=True) + 1e-12)
    quat_a = quaternion[0]
    quat_b = quaternion[1]
    quat_c = quaternion[2]
    quat_d = quaternion[3]
    spin = jnp.stack([quat_a * quat_a + quat_b * quat_b - quat_c * quat_c - quat_d * quat_d, 2.0 * (quat_b * quat_c - quat_a * quat_d), 2.0 * (quat_b * quat_d + quat_a * quat_c), 2.0 * (quat_b * quat_c + quat_a * quat_d), quat_a * quat_a - quat_b * quat_b + quat_c * quat_c - quat_d * quat_d, 2.0 * (quat_c * quat_d - quat_a * quat_b), 2.0 * (quat_b * quat_d - quat_a * quat_c), 2.0 * (quat_c * quat_d + quat_a * quat_b), quat_a * quat_a - quat_b * quat_b - quat_c * quat_c + quat_d * quat_d])
    steps = jax.random.normal(key_walk, (3, N_RES), jnp.float32) * 2.2
    walk = jnp.cumsum(steps, axis=1)
    walk = walk - jnp.mean(walk, axis=1, keepdims=True)
    return jnp.concatenate([spin, walk], axis=0).astype(jnp.float32)


def plant(array, stream_key, smallest, high):
    longest = array.shape.index(max(array.shape))
    spots = []
    for shift in (0, 1):
        where = [jax.random.randint(jax.random.fold_in(stream_key, axis), (), 0, length) for axis, length in enumerate(array.shape)]
        where[longest] = (where[longest] + shift) % array.shape[longest]
        spots.append(tuple(where))
    return array.at[spots[0]].set(smallest).at[spots[1]].set(high)


def block_scale(own_key, dims, cuts, least, largest):
    loudness = 1.0
    for dim, blocks in cuts:
        draws = jax.random.uniform(jax.random.fold_in(jax.random.fold_in(own_key, 6), dim), (blocks,), jnp.float32, least / len(cuts), largest / len(cuts))
        loudness = loudness * jnp.repeat(jnp.exp(draws), dims[dim] // blocks).reshape((-1,) + (1,) * (len(dims) - 1 - dim))
    return loudness


def length_profile(number_of, total, limit, slope):
    weights = [(1 << 20) // math.isqrt(rank ** slope) + 1 for rank in range(2, number_of + 1)]
    rest, counts = total - limit - (number_of - 1), [1] * (number_of - 1)
    while rest > 0:
        candidates = [i for i in range(number_of - 1) if counts[i] < limit]
        mass, left = sum([weights[i] for i in candidates]), rest
        for i in candidates:
            addition = min(limit - counts[i], max(1, left * weights[i] // mass), rest)
            counts[i] = counts[i] + addition
            rest = rest - addition
    return np.array([limit] + counts)


def uneven_parts(stream_key, number_of, total, limit, slope):
    if number_of == 2:
        one = jax.random.randint(stream_key, (), max(1, total - limit), min(limit, total - 1) + 1)
        return jnp.stack([one, total - one])
    tallies = jnp.asarray(length_profile(number_of, total, limit, slope), jnp.int32)
    twos = (number_of - 1) // 2
    source_of, taker = tallies[1:1 + 2 * twos:2], tallies[2:2 + 2 * twos:2]
    slack = jnp.minimum(source_of - 1, limit - taker)
    moved = jax.random.randint(jax.random.fold_in(stream_key, 1), (twos,), 0, 1 << 20) % (slack + 1)
    tallies = tallies.at[1:1 + 2 * twos:2].set(source_of - moved).at[2:2 + 2 * twos:2].set(taker + moved)
    return tallies[jax.random.permutation(jax.random.fold_in(stream_key, 2), number_of)]


def scatter_about(own_key, extent, scale, bound, split=(), held_as=jnp.bfloat16):
    entries = scale * jax.random.normal(own_key, extent, jnp.float32)
    if split:
        entries = entries * block_scale(own_key, extent, split, -0.22, 0.18)
    return jnp.clip(entries, -bound, bound).astype(held_as)


def setup_inputs(seed: int = 0, part: int = 0) -> dict:
    arg_keys = jax.random.split(jax.random.key(seed), 16)
    part_keys = jax.random.split(jax.random.fold_in(arg_keys[15], part), 16)
    single = scatter_about(part_keys[0], (N_RES, C), 1.0, 6.0, ((0, 32),))
    pair = scatter_about(part_keys[1], (N_RES, KEY_BLOCKS, ROW_DEV, CZ), 1.0, 6.0, ((0, 32), (2, 2)))
    frames = draw_frames(jax.random.fold_in(jax.random.fold_in(arg_keys[15], part), 71), part)
    chain = jnp.searchsorted(jnp.cumsum(uneven_parts(part_keys[3], 6, N_RES, N_RES // 3, 0)), jnp.arange(N_RES), side="right").astype(jnp.int32)
    mask = plant((jax.random.randint(part_keys[4], (N_RES,), 0, 8) < 7).astype(jnp.int32), jax.random.fold_in(part_keys[4], 1), 0, 1)
    w_query = scatter_about(arg_keys[5], (C, HEADS * CH), C ** -0.5, 0.3125, ((1, 4),))
    w_key_value = scatter_about(arg_keys[6], (C, HEADS * 2 * CH), C ** -0.5, 0.3125, ((1, 4),))
    w_query_points = scatter_about(arg_keys[7], (C, HEADS * PQ * 3), C ** -0.5, 0.3125, ((1, 4),))
    w_kv_points = scatter_about(arg_keys[8], (C, HEADS * (PQ + PV) * 3), C ** -0.5, 0.3125, ((1, 4),))
    w_pair_bias = scatter_about(arg_keys[9], (CZ, HEADS), CZ ** -0.5, 0.5, ((1, 4),))
    head_weights = jnp.clip(-9.0 + 10.0 * jax.random.uniform(arg_keys[10], (HEADS,), jnp.float32) ** block_scale(arg_keys[10], (HEADS,), ((0, 4),), -0.2, 0.2), -9.0, 1.0)
    chain_bias = jnp.clip(jax.random.uniform(arg_keys[11], (HEADS,), jnp.float32, -3.0, 3.0) * block_scale(arg_keys[11], (HEADS,), ((0, 4),), -0.4, 0.0), -3.0, 3.0)
    w_out = scatter_about(arg_keys[12], (HEADS, CAT, C), (HEADS * CAT) ** -0.5, 0.125, ((0, 4),))
    out_gain = jnp.clip(1.0 + 0.1 * jax.random.normal(arg_keys[13], (C,), jnp.float32), 0.5, 1.5)
    w_backbone = scatter_about(arg_keys[14], (C, 6), C ** -0.5, 0.3125)
    return dict(single=single, pair=pair, frames=frames, chain=chain, mask=mask, w_query=w_query, w_key_value=w_key_value, w_query_points=w_query_points, w_kv_points=w_kv_points, w_pair_bias=w_pair_bias, head_weights=head_weights, chain_bias=chain_bias, w_out=w_out, out_gain=out_gain, w_backbone=w_backbone)


HIGH = lax.Precision.HIGHEST
LOGIT_WEIGHT = math.sqrt(1.0 / 3.0)
MASK_PENALTY = 100000.0

def to_global(local, frames):
    rotation = frames[:9].reshape(3, 3, -1)
    moved = jnp.einsum('abn,ngb->nga', rotation, local, precision=HIGH)
    return moved + jnp.transpose(frames[9:12])[:, None, :]

def to_local(points, frames):
    rotation = frames[:9].reshape(3, 3, -1)
    moved = points - jnp.transpose(frames[9:12])[:, None, None, :]
    return jnp.einsum('abn,nhpa->nhpb', rotation, moved, precision=HIGH)

def compose(frames, motion):
    rotation = frames[:9].reshape(3, 3, -1)
    inverse = 1.0 / jnp.sqrt(1.0 + motion[:, 0] ** 2 + motion[:, 1] ** 2 + motion[:, 2] ** 2)
    quat_a = inverse
    quat_b = motion[:, 0] * inverse
    quat_c = motion[:, 1] * inverse
    quat_d = motion[:, 2] * inverse
    spin = jnp.stack([quat_a * quat_a + quat_b * quat_b - quat_c * quat_c - quat_d * quat_d, 2.0 * (quat_b * quat_c - quat_a * quat_d), 2.0 * (quat_b * quat_d + quat_a * quat_c), 2.0 * (quat_b * quat_c + quat_a * quat_d), quat_a * quat_a - quat_b * quat_b + quat_c * quat_c - quat_d * quat_d, 2.0 * (quat_c * quat_d - quat_a * quat_b), 2.0 * (quat_b * quat_d - quat_a * quat_c), 2.0 * (quat_c * quat_d + quat_a * quat_b), quat_a * quat_a - quat_b * quat_b - quat_c * quat_c + quat_d * quat_d]).reshape(3, 3, -1)
    new_rotation = jnp.einsum('abn,bcn->acn', rotation, spin, precision=HIGH)
    offset = jnp.einsum('abn,nb->an', rotation, motion[:, 3:6], precision=HIGH)
    return jnp.concatenate([new_rotation.reshape(9, -1), frames[9:12] + offset], axis=0)

def attention_logits(pair_rows, query_rows, query_points, query_chain, query_present, keys, key_points, key_chain, key_present, w_pair_bias, distance_scale, chain_bias):
    count_q = pair_rows.shape[0]
    count_k = pair_rows.shape[1]
    bias = jnp.dot(pair_rows.reshape(count_q * count_k, -1), w_pair_bias, preferred_element_type=jnp.float32).reshape(count_q, count_k, -1)
    dots = jnp.einsum('ihc,jhc->ijh', query_rows, keys, precision=HIGH) / math.sqrt(keys.shape[-1])
    gaps = query_points[:, None] - key_points[None]
    distance = lax.optimization_barrier(jnp.sum(gaps * gaps, axis=(3, 4)))
    differ = (query_chain[:, None] != key_chain[None, :]).astype(jnp.float32)
    logits = LOGIT_WEIGHT * (dots + bias - distance_scale * distance + chain_bias * differ[..., None])
    absent = 1.0 - query_present[:, None] * key_present[None, :]
    return logits - MASK_PENALTY * absent[..., None]

def reference(single, pair, frames, chain, mask, w_query, w_key_value, w_query_points, w_kv_points, w_pair_bias, head_weights, chain_bias, w_out, out_gain, w_backbone):
    count = N_RES
    query = jnp.dot(single, w_query, preferred_element_type=jnp.float32).reshape(count, HEADS, CH)
    key_value = jnp.dot(single, w_key_value, preferred_element_type=jnp.float32).reshape(count, HEADS, 2, CH)
    keys = key_value[:, :, 0]
    values = key_value[:, :, 1]
    query_local = jnp.dot(single, w_query_points, preferred_element_type=jnp.float32).reshape(count, HEADS * PQ, 3)
    query_points = to_global(query_local, frames).reshape(count, HEADS, PQ, 3)
    pair_local = jnp.dot(single, w_kv_points, preferred_element_type=jnp.float32).reshape(count, HEADS * (PQ + PV), 3)
    point_pairs = to_global(pair_local, frames).reshape(count, HEADS, PQ + PV, 3)
    key_points = point_pairs[:, :, :PQ]
    value_points = point_pairs[:, :, PQ:]
    distance_scale = jax.nn.softplus(head_weights) * math.sqrt(2.0 / (9.0 * PQ)) / 2.0
    chain_float = chain.astype(jnp.float32)
    present = mask.astype(jnp.float32)
    pair_flat = pair.reshape(count, count, CZ)
    w_flat = w_out.reshape(HEADS * CAT, C)

    def block_rows(start):
        pair_rows = lax.dynamic_slice_in_dim(pair_flat, start, ROW_DEV, 0)
        query_rows = lax.dynamic_slice_in_dim(query, start, ROW_DEV, 0)
        qpoint_rows = lax.dynamic_slice_in_dim(query_points, start, ROW_DEV, 0)
        chain_rows = lax.dynamic_slice_in_dim(chain_float, start, ROW_DEV, 0)
        present_rows = lax.dynamic_slice_in_dim(present, start, ROW_DEV, 0)
        frame_rows = lax.dynamic_slice_in_dim(frames, start, ROW_DEV, 1)
        logits = attention_logits(pair_rows, query_rows, qpoint_rows, chain_rows, present_rows, keys, key_points, chain_float, present, w_pair_bias, distance_scale, chain_bias)
        top = lax.optimization_barrier(jnp.max(logits, axis=1))
        weights = jnp.exp(logits - top[:, None, :])
        total = lax.optimization_barrier(jnp.sum(weights, axis=1))
        attended = jnp.einsum('ijh,jhc->ihc', weights, values, precision=HIGH) / total[..., None]
        pointed_global = jnp.einsum('ijh,jhpd->ihpd', weights, value_points, precision=HIGH) / total[..., None, None]
        rounded = lax.optimization_barrier(weights.astype(jnp.bfloat16)).astype(jnp.float32)
        paired = jnp.einsum('ijh,ijc->ihc', rounded, pair_rows.astype(jnp.float32), precision=HIGH) / total[..., None]
        pointed = to_local(pointed_global, frame_rows)
        point_norms = jnp.sqrt(lax.optimization_barrier(jnp.sum(pointed * pointed, axis=3)) + 1.0)
        joined = jnp.concatenate([attended, pointed.reshape(ROW_DEV, HEADS, PV * 3), point_norms, paired], axis=2).astype(jnp.bfloat16)
        return jnp.dot(joined.reshape(ROW_DEV, HEADS * CAT), w_flat, preferred_element_type=jnp.float32)
    starts = jnp.arange(N_BLK, dtype=jnp.int32) * ROW_DEV
    update = lax.map(block_rows, starts).reshape(count, C)
    mixed = single.astype(jnp.float32) + update
    centre = lax.optimization_barrier(jnp.mean(mixed, axis=1, keepdims=True))
    spread = lax.optimization_barrier(jnp.mean(jnp.square(mixed - centre), axis=1, keepdims=True))
    single_out = ((mixed - centre) * lax.rsqrt(spread + 1e-05) * out_gain).astype(jnp.bfloat16)
    motion = jnp.dot(single_out, w_backbone, preferred_element_type=jnp.float32)
    frames_out = compose(frames, motion)
    return (single_out, frames_out)
```

```python
import functools
import math

import jax
import jax.numpy as jnp
from jax import lax
from jax.experimental import pallas as pl
from jax.experimental.pallas import tpu as pltpu
from jax.sharding import Mesh
from jax.sharding import PartitionSpec as P

HIGH = lax.Precision.HIGHEST
LOGIT_WEIGHT = math.sqrt(1.0 / 3.0)
MASK_PENALTY = 100000.0
F32 = jnp.float32
BF16 = jnp.bfloat16

SLOTS = 4
HALF = 128
COMP = 40
CHAIN, PRESENT, ONE, TOP = 120, 121, 122, 123
VMEM = pl.BlockSpec(memory_space=pltpu.VMEM)
SMEM = pl.BlockSpec(memory_space=pltpu.SMEM)


def iota(shape, dim):
    return lax.broadcasted_iota(jnp.int32, shape, dim)


def dot(a, b, precision=None):
    return jnp.dot(a, b, preferred_element_type=F32, precision=precision)


def rotated(frames_ref, parts):
    moved = []
    for a in range(3):
        total = frames_ref[3 * a : 3 * a + 1, :] * parts[0]
        for b in (1, 2):
            total += frames_ref[3 * a + b : 3 * a + b + 1, :] * parts[b]
        moved.append(total + frames_ref[9 + a : 10 + a, :])
    return moved


def project_kernel(
    heads,
    size,
    n_query,
    n_points,
    single_ref,
    frames_ref,
    chain_ref,
    mask_ref,
    wq_ref,
    wkv_ref,
    wqp_ref,
    wkp_ref,
    hw_ref,
    cb_ref,
    payload_ref,
    qb_ref,
    qaux_ref,
    frows_ref,
    flat,
    turned,
    points,
    full,
    spread,
):
    rows = single_ref.shape[0]
    half = payload_ref.shape[0]
    x = single_ref[...]
    q_wide = heads * size
    flat[...] = jnp.zeros_like(flat)
    flat[:, 0:q_wide] = dot(x, wq_ref[...])
    flat[:, HALF : HALF + 3 * heads * n_query] = dot(x, wqp_ref[...])
    flat[:, 2 * HALF : 2 * HALF + 3 * heads * n_points] = dot(x, wkp_ref[...])
    full[...] = jnp.zeros_like(full)
    full[:, 0 : 2 * q_wide] = dot(x, wkv_ref[...])
    for k in range(3):
        turned[k * HALF : (k + 1) * HALF, :] = flat[:, k * HALF : (k + 1) * HALF].T
    chain_row = chain_ref[...].astype(F32).reshape(1, rows)
    mask_row = mask_ref[...].astype(F32).reshape(1, rows)

    count = heads * n_points
    local = [turned[pl.ds(2 * HALF + b, count, stride=3), :] for b in range(3)]
    points[...] = jnp.zeros_like(points)
    for a, value in enumerate(rotated(frames_ref, local)):
        points[COMP * a : COMP * a + count, :] = value
    points[CHAIN : CHAIN + 1, :] = chain_row
    points[PRESENT : PRESENT + 1, :] = mask_row
    points[ONE : ONE + 1, :] = jnp.ones((1, rows), F32)
    full[:, HALF:] = points[...].T
    start = pl.multiple_of(lax.axis_index("pair") * half, half)
    payload_ref[...] = full[pl.ds(start, half), :]

    count = heads * n_query
    local = [turned[pl.ds(HALF + b, count, stride=3), :] for b in range(3)]
    spread[...] = jnp.zeros_like(spread)
    spread[0:q_wide, :] = turned[0:q_wide, :]
    for a, value in enumerate(rotated(frames_ref, local)):
        spread[48 + 16 * a : 48 + 16 * a + count, :] = value
    spread[96:97, :] = chain_row
    spread[97:98, :] = mask_row
    to_slots = (iota((rows, HALF), 1) // SLOTS == iota((rows, HALF), 0)).astype(F32)
    wide = dot(spread[...], to_slots, HIGH)
    slot = iota((1, HALF), 1) % SLOTS
    qb_ref[...] = jnp.zeros_like(qb_ref)
    scale = LOGIT_WEIGHT / math.sqrt(size)
    for h in range(heads):
        block = wide[h * size : (h + 1) * size, :] * scale
        qb_ref[2 * size * h : 2 * size * h + size, :] = jnp.where(slot == h, block, 0.0)
    qaux_ref[...] = jnp.zeros_like(qaux_ref)
    for a in range(3):
        for p in range(n_query):
            line = jnp.zeros((1, HALF), F32)
            for h in range(heads):
                at = 48 + 16 * a + h * n_query + p
                line = jnp.where(slot == h, wide[at : at + 1, :], line)
            qaux_ref[n_query * a + p : n_query * a + p + 1, :] = line
    raw = jnp.zeros((1, HALF), F32)
    bonus = jnp.zeros((1, HALF), F32)
    for h in range(heads):
        raw = jnp.where(slot == h, hw_ref[h], raw)
        bonus = jnp.where(slot == h, cb_ref[h], bonus)
    soft = jnp.maximum(raw, 0.0) + jnp.log1p(jnp.exp(-jnp.abs(raw)))
    used = 3 * n_query
    qaux_ref[used : used + 1, :] = soft * (math.sqrt(2.0 / (9.0 * n_query)) / 2.0)
    qaux_ref[used + 1 : used + 2, :] = bonus
    qaux_ref[used + 2 : used + 3, :] = wide[96:97, :]
    qaux_ref[used + 3 : used + 4, :] = wide[97:98, :]

    points[...] = jnp.zeros_like(points)
    points[0:12, :] = frames_ref[...]
    columns = points[...].T
    to_rows = (iota((HALF, rows), 0) // SLOTS == iota((HALF, rows), 1)).astype(F32)
    frows_ref[...] = dot(to_rows, columns, HIGH)


def bias_kernel(heads, pair_ref, wb_ref, bias_ref, weights):
    queries = pair_ref.shape[0]
    width = pair_ref.shape[3]
    keys = pair_ref.shape[1] * pair_ref.shape[2]
    lane = iota((width, HALF), 1)
    wb = wb_ref[...].astype(F32)
    each = jnp.zeros((width, HALF), F32)
    for h in range(heads):
        each = jnp.where(lane % SLOTS == h, wb[:, h : h + 1], each)
    for i in range(queries):
        weights[i * width : (i + 1) * width, :] = jnp.where(
            lane // SLOTS == i, each, 0.0
        ).astype(BF16)
    left = jnp.concatenate([pair_ref[i].reshape(keys, width) for i in range(queries)], axis=1)
    bias_ref[...] = dot(left, weights[...])


def attend_kernel(
    n_query, payload_ref, bias_ref, qb_ref, qaux_ref, pair_ref, part_ref, turned_w
):
    near, far, half, lanes = payload_ref.shape
    keys = near * far * half
    queries = pair_ref.shape[0]
    width = pair_ref.shape[3]
    block = jnp.concatenate(
        [payload_ref[k % near, k // near] for k in range(near * far)], axis=0
    )
    high = block[:, HALF:]
    first = high.astype(BF16)
    rest = high - first.astype(F32)
    second = rest.astype(BF16)
    third = (rest - second.astype(F32)).astype(BF16)
    split = jnp.concatenate([first, second, third], axis=1)

    row = iota((HALF, HALF), 0)
    lane = iota((HALF, HALF), 1)
    slot = lane % SLOTS

    def expanded(wanted):
        picks = (row == wanted).astype(F32).astype(BF16)
        return dot(split, jnp.concatenate([picks, picks, picks], axis=0))

    distance = jnp.zeros((keys, HALF), F32)
    for a in range(3):
        for p in range(n_query):
            wanted = jnp.where(slot < 3, COMP * a + 12 * slot + p, -1)
            at = n_query * a + p
            gap = qaux_ref[at : at + 1, :] - expanded(wanted)
            distance += gap * gap
    used = 3 * n_query
    scale = qaux_ref[used : used + 1, :]
    bonus = qaux_ref[used + 1 : used + 2, :]
    differ = expanded(jnp.full((HALF, HALF), CHAIN)) != qaux_ref[used + 2 : used + 3, :]
    there = expanded(jnp.full((HALF, HALF), PRESENT)) * qaux_ref[used + 3 : used + 4, :]
    logits = dot(block[:, :HALF], qb_ref[...], HIGH) + LOGIT_WEIGHT * (
        bias_ref[...] - scale * distance + jnp.where(differ, bonus, 0.0)
    )
    logits = logits - MASK_PENALTY * (1.0 - there)
    by_row = logits.T
    top = jnp.max(by_row, axis=1, keepdims=True)
    weights = jnp.exp(by_row - top)
    turned_w[...] = weights
    sums = dot(weights, block, HIGH)
    part_ref[:, HALF:] = jnp.where(iota((HALF, lanes), 1) == HALF + TOP, top, sums)
    upper = iota((2 * SLOTS, width), 0) < SLOTS
    for g in range(queries // 2):
        rows = slice(2 * SLOTS * g, 2 * SLOTS * (g + 1))
        right = jnp.concatenate(
            [pair_ref[2 * g].reshape(keys, width), pair_ref[2 * g + 1].reshape(keys, width)],
            axis=1,
        )
        both = dot(turned_w[rows, :].astype(BF16), right)
        part_ref[rows, 0:width] = jnp.where(upper, both[:, :width], both[:, width:])


def merge_kernel(
    heads,
    size,
    n_query,
    n_value,
    mine_ref,
    theirs_ref,
    frows_ref,
    w_out_ref,
    out_ref,
    small,
    large,
):
    copies, rows, _ = out_ref.shape
    tops = [ref[:, 2 * HALF + TOP : 2 * HALF + TOP + 1] for ref in (mine_ref, theirs_ref)]
    sums = [ref[:, 2 * HALF + ONE : 2 * HALF + ONE + 1] for ref in (mine_ref, theirs_ref)]
    best = jnp.maximum(tops[0], tops[1])
    factors = [jnp.exp(top - best) for top in tops]
    total = factors[0] * sums[0] + factors[1] * sums[1]
    merged = (mine_ref[...] * factors[0] + theirs_ref[...] * factors[1]) / total
    slot = iota((HALF, 1), 0) % SLOTS

    def of_own_head(first, step, count):
        picked = jnp.zeros((HALF, count), F32)
        for h in range(heads):
            at = first + step * h
            picked = jnp.where(slot == h, merged[:, at : at + count], picked)
        return picked

    attended = of_own_head(HALF + size, 2 * size, size)
    n_points = n_query + n_value
    moved = [
        of_own_head(2 * HALF + COMP * a + n_query, n_points, n_value)
        - frows_ref[:, 9 + a : 10 + a]
        for a in range(3)
    ]
    pointed = []
    for b in range(3):
        total_b = frows_ref[:, b : b + 1] * moved[0]
        for a in (1, 2):
            total_b += frows_ref[:, 3 * a + b : 3 * a + b + 1] * moved[a]
        pointed.append(total_b)
    norms = jnp.sqrt(
        pointed[0] * pointed[0] + pointed[1] * pointed[1] + pointed[2] * pointed[2] + 1.0
    )
    small[...] = jnp.zeros_like(small)
    small[:, 0:size] = attended
    for b in range(3):
        small[:, size + n_value * b : size + n_value * (b + 1)] = pointed[b]
    edge = size + 3 * n_value
    small[:, edge : edge + n_value] = norms
    source = iota((HALF, HALF), 0)
    target = iota((HALF, HALF), 1)
    inside = (source >= size) & (source < edge)
    goes = jnp.where(
        inside, size + 3 * ((source - size) % n_value) + (source - size) // n_value, source
    )
    order = (goes == target).astype(F32).astype(BF16)
    small[...] = dot(small[...].astype(BF16), order)
    large[...] = merged[:, :HALF]
    cut = edge + n_value
    update = jnp.zeros((rows, w_out_ref.shape[2]), F32)
    for h in range(heads):
        low = small[pl.ds(h, rows, stride=SLOTS), :].astype(BF16)
        update += dot(low[:, :cut], w_out_ref[h, 0:cut, :])
        wide = large[pl.ds(h, rows, stride=SLOTS), :].astype(BF16)
        update += dot(wide, w_out_ref[h, cut:, :])
    for k in range(copies):
        out_ref[k] = update


def finish_kernel(updates_ref, single_ref, gain_ref, wb_ref, frames_ref, out_ref, send_ref, flat):
    copies, rows, channels = updates_ref.shape
    mixed = single_ref[...].astype(F32)
    update = updates_ref[0]
    for k in range(1, copies):
        update += updates_ref[k]
    mixed = mixed + update
    centre = jnp.mean(mixed, axis=1, keepdims=True)
    away = mixed - centre
    spread = jnp.mean(away * away, axis=1, keepdims=True)
    gain = gain_ref[...].reshape(1, channels)
    single_out = (away * lax.rsqrt(spread + 1e-05) * gain).astype(BF16)
    out_ref[...] = single_out
    flat[...] = jnp.zeros_like(flat)
    flat[:, 0:6] = dot(single_out, wb_ref[...])
    motion = flat[...].T
    m = [motion[k : k + 1, :] for k in range(6)]
    qa = 1.0 / jnp.sqrt(1.0 + m[0] * m[0] + m[1] * m[1] + m[2] * m[2])
    qb, qc, qd = m[0] * qa, m[1] * qa, m[2] * qa
    spin = [
        [qa * qa + qb * qb - qc * qc - qd * qd, 2.0 * (qb * qc - qa * qd), 2.0 * (qb * qd + qa * qc)],
        [2.0 * (qb * qc + qa * qd), qa * qa - qb * qb + qc * qc - qd * qd, 2.0 * (qc * qd - qa * qb)],
        [2.0 * (qb * qd - qa * qc), 2.0 * (qc * qd + qa * qb), qa * qa - qb * qb - qc * qc + qd * qd],
    ]
    r = [[frames_ref[3 * a + b : 3 * a + b + 1, :] for b in range(3)] for a in range(3)]
    lines = []
    for a in range(3):
        for c in range(3):
            lines.append(r[a][0] * spin[0][c] + r[a][1] * spin[1][c] + r[a][2] * spin[2][c])
    for a in range(3):
        lines.append(
            frames_ref[9 + a : 10 + a, :] + (r[a][0] * m[3] + r[a][1] * m[4] + r[a][2] * m[5])
        )
    groups = HALF // rows
    repeat = (iota((rows, HALF), 1) % rows == iota((rows, HALF), 0)).astype(F32)
    wide = dot(jnp.concatenate(lines + lines[:4], axis=0), repeat, HIGH)
    group = iota((1, HALF), 1) // rows
    pieces = []
    for v in range(len(lines) // groups):
        piece = wide[groups * v : groups * v + 1, :]
        for s in range(1, groups):
            at = groups * v + s
            piece = jnp.where(group == s, wide[at : at + 1, :], piece)
        pieces.append(piece)
    line = jnp.concatenate(pieces, axis=1)
    send_ref[...] = jnp.broadcast_to(line, (send_ref.shape[0], line.shape[1])).reshape(
        send_ref.shape
    )


def spread_kernel(blocks_ref, out_ref):
    blocks, _, wide = blocks_ref.shape
    lines = out_ref.shape[0]
    rows = wide // lines
    groups = HALF // rows
    x = blocks_ref[...].reshape(blocks, wide)
    s = iota((blocks, HALF), 0) % groups
    g = iota((blocks, HALF), 1) // rows
    for v in range(wide // HALF):
        tile = x[:, HALF * v : HALF * (v + 1)]
        z = tile
        for d in range(1, groups):
            right = pltpu.roll(tile, rows * d, 1)
            up = pltpu.roll(right, blocks - d, 0)
            down = pltpu.roll(right, groups - d, 0)
            z = jnp.where(g - s == d, up, z)
            z = jnp.where(g - s == d - groups, down, z)
        for q in range(blocks // groups):
            out_ref[groups * v : groups * (v + 1), HALF * q : HALF * (q + 1)] = z[
                groups * q : groups * (q + 1), :
            ]


def call(kernel, outs, scratch=(), specs=None, n=0, cost=None, name=None):
    return pl.pallas_call(
        kernel,
        out_shape=outs,
        in_specs=specs or [VMEM] * n,
        out_specs=jax.tree.map(lambda _: VMEM, outs),
        scratch_shapes=list(scratch),
        cost_estimate=cost,
        name=name,
    )


def body(
    single,
    pair,
    frames,
    chain,
    mask,
    w_query,
    w_key_value,
    w_query_points,
    w_kv_points,
    w_pair_bias,
    head_weights,
    chain_bias,
    w_out,
    out_gain,
    w_backbone,
):
    rows, channels = single.shape
    blocks, half = pair.shape[1], pair.shape[2]
    width = pair.shape[3]
    heads = w_pair_bias.shape[1]
    size = w_query.shape[1] // heads
    n_query = w_query_points.shape[1] // (3 * heads)
    n_points = w_kv_points.shape[1] // (3 * heads)
    n_value = n_points - n_query
    keys = blocks * half
    shape = jax.ShapeDtypeStruct

    payload, qb, qaux, frows = call(
        functools.partial(project_kernel, heads, size, n_query, n_points),
        (
            shape((half, 2 * HALF), F32),
            shape((HALF, HALF), F32),
            shape((16, HALF), F32),
            shape((HALF, HALF), F32),
        ),
        (
            pltpu.VMEM((rows, 3 * HALF), F32),
            pltpu.VMEM((3 * HALF, rows), F32),
            pltpu.VMEM((HALF, rows), F32),
            pltpu.VMEM((rows, 2 * HALF), F32),
            pltpu.VMEM((104, rows), F32),
        ),
        specs=[VMEM] * 8 + [SMEM] * 2,
        name="project",
    )(
        single,
        frames,
        chain,
        mask,
        w_query,
        w_key_value,
        w_query_points,
        w_kv_points,
        head_weights,
        chain_bias,
    )
    gathered = lax.all_gather(payload, "far", axis=0, tiled=False)
    gathered = lax.all_gather(gathered, "near", axis=0, tiled=False)
    bias = call(
        functools.partial(bias_kernel, heads),
        shape((keys, HALF), F32),
        (pltpu.VMEM((rows * width, HALF), BF16),),
        n=2,
        name="bias",
    )(pair, w_pair_bias)
    part = call(
        functools.partial(attend_kernel, n_query),
        shape((HALF, 3 * HALF), F32),
        (pltpu.VMEM((HALF, keys), F32),),
        n=5,
        name="attend",
    )(gathered, bias, qb, qaux, pair)
    swap = [(k, 1 - k) for k in range(2)]
    other = lax.ppermute(part, "pair", swap)
    updates = call(
        functools.partial(merge_kernel, heads, size, n_query, n_value),
        shape((lax.axis_size("head"), rows, channels), F32),
        (pltpu.VMEM((HALF, HALF), F32), pltpu.VMEM((HALF, HALF), F32)),
        n=4,
        name="merge",
    )(part, other, frows, w_out)
    updates = lax.all_to_all(updates, "head", split_axis=0, concat_axis=0, tiled=True)
    single_out, send = call(
        finish_kernel,
        (shape((rows, channels), BF16), shape((blocks, 1, 12 * rows), F32)),
        (pltpu.VMEM((rows, HALF), F32),),
        n=5,
        name="finish",
    )(updates, single, out_gain, w_backbone, frames)
    received = lax.all_to_all(send, ("far", "near"), split_axis=0, concat_axis=0, tiled=True)
    frames_out = call(
        spread_kernel, shape((12, blocks * rows), F32), n=1, name="spread"
    )(received)
    return (single_out, frames_out)


def solution(mesh):
    groups, blocks, heads, pairs = (mesh.shape[a] for a in ("groups", "blk", "head", "pair"))
    near = 2 if blocks % 2 == 0 else 1
    finer = Mesh(
        mesh.devices.reshape(groups, blocks // near, near, heads, pairs),
        ("groups", "far", "near", "head", "pair"),
    )
    split = ("groups", "far", "near")
    placed = (
        P(split, None),
        P(split, None, "pair", None),
        P(None, split),
        P(split),
        P(split),
        P(None, "head"),
        P(None, "head"),
        P(None, "head"),
        P(None, "head"),
        P(None, "head"),
        P("head"),
        P("head"),
        P("head", None, None),
        P(),
        P(),
    )
    return jax.shard_map(
        body,
        mesh=finer,
        in_specs=placed,
        out_specs=(P(split, None), P(None, "groups")),
        check_vma=False,
    )
```

```python
import functools
import math

import jax
import jax.numpy as jnp
from jax import lax
from jax.experimental import pallas as pl
from jax.experimental.pallas import tpu as pltpu
from jax.sharding import Mesh
from jax.sharding import PartitionSpec as P

HIGH = lax.Precision.HIGHEST
LOGIT_WEIGHT = math.sqrt(1.0 / 3.0)
MASK_PENALTY = 100000.0
F32 = jnp.float32
BF16 = jnp.bfloat16

SLOTS = 4
HALF = 128
BIAS_STEPS = 4
COMP = 40
CHAIN, PRESENT, ONE, TOP = 120, 121, 122, 123
VMEM = pl.BlockSpec(memory_space=pltpu.VMEM)
HBM = pl.BlockSpec(memory_space=pltpu.HBM)


def iota(shape, dim):
    return lax.broadcasted_iota(jnp.int32, shape, dim)


def dot(a, b, precision=None):
    return jnp.dot(a, b, preferred_element_type=F32, precision=precision)


def dot_nt(a, b):
    return lax.dot_general(a, b, (((1,), (1,)), ((), ())), preferred_element_type=F32)


def rotated(frames_ref, parts):
    moved = []
    for a in range(3):
        total = frames_ref[3 * a : 3 * a + 1, :] * parts[0]
        for b in (1, 2):
            total += frames_ref[3 * a + b : 3 * a + b + 1, :] * parts[b]
        moved.append(total + frames_ref[9 + a : 10 + a, :])
    return moved


def project_kernel(
    heads,
    size,
    n_query,
    n_points,
    *refs,
):
    sources, refs = refs[:10], refs[10:]
    payload_ref, qb_ref, qaux_ref, frows_ref, turned, points, full, spread = refs[:8]
    local_refs, sem = refs[8:18], refs[18]
    copies = [
        pltpu.make_async_copy(source, target, sem.at[k])
        for k, (source, target) in enumerate(zip(sources, local_refs))
    ]
    for copy in copies:
        copy.start()
    single_ref, frames_ref, chain_ref, mask_ref, wq_ref, wkv_ref, wqp_ref, wkp_ref = local_refs[:8]
    hw_ref, cb_ref = local_refs[8:]
    full[...] = jnp.zeros_like(full)
    points[...] = jnp.zeros_like(points)
    spread[...] = jnp.zeros_like(spread)
    qb_ref[...] = jnp.zeros_like(qb_ref)
    qaux_ref[...] = jnp.zeros_like(qaux_ref)
    for copy in copies:
        copy.wait()
    rows = single_ref.shape[0]
    half = payload_ref.shape[0]
    x = single_ref[...]
    q_wide = heads * size
    turned[HALF : HALF + 3 * heads * n_query, :] = dot_nt(wqp_ref[...], x)
    turned[2 * HALF : 2 * HALF + 3 * heads * n_points, :] = dot_nt(wkp_ref[...], x)
    full[:, 0 : 2 * q_wide] = dot_nt(x, wkv_ref[...])
    chain_row = chain_ref[...].astype(F32).reshape(1, rows)
    mask_row = mask_ref[...].astype(F32).reshape(1, rows)

    count = heads * n_points
    local = [turned[pl.ds(2 * HALF + b, count, stride=3), :] for b in range(3)]
    for a, value in enumerate(rotated(frames_ref, local)):
        points[COMP * a : COMP * a + count, :] = value
    points[CHAIN : CHAIN + 1, :] = chain_row
    points[PRESENT : PRESENT + 1, :] = mask_row
    points[ONE : ONE + 1, :] = jnp.ones((1, rows), F32)
    full[:, HALF:] = points[...].T
    start = pl.multiple_of(lax.axis_index("pair") * half, half)
    payload_ref[...] = full[pl.ds(start, half), :]

    count = heads * n_query
    local = [turned[pl.ds(HALF + b, count, stride=3), :] for b in range(3)]
    spread[0:q_wide, :] = dot_nt(wq_ref[...], x)
    for a, value in enumerate(rotated(frames_ref, local)):
        spread[48 + 16 * a : 48 + 16 * a + count, :] = value
    spread[96:97, :] = chain_row
    spread[97:98, :] = mask_row
    to_slots = (iota((rows, HALF), 1) // SLOTS == iota((rows, HALF), 0)).astype(F32)
    wide = dot(spread[...], to_slots, HIGH)
    slot = iota((1, HALF), 1) % SLOTS
    scale = LOGIT_WEIGHT / math.sqrt(size)
    for h in range(heads):
        block = wide[h * size : (h + 1) * size, :] * scale
        qb_ref[2 * size * h : 2 * size * h + size, :] = jnp.where(slot == h, block, 0.0)
    for a in range(3):
        for p in range(n_query):
            line = jnp.zeros((1, HALF), F32)
            for h in range(heads):
                at = 48 + 16 * a + h * n_query + p
                line = jnp.where(slot == h, wide[at : at + 1, :], line)
            qaux_ref[n_query * a + p : n_query * a + p + 1, :] = line
    raw = jnp.zeros((1, HALF), F32)
    bonus = jnp.zeros((1, HALF), F32)
    for h in range(heads):
        raw = jnp.where(slot == h, hw_ref[h], raw)
        bonus = jnp.where(slot == h, cb_ref[h], bonus)
    soft = jnp.maximum(raw, 0.0) + jnp.log1p(jnp.exp(-jnp.abs(raw)))
    used = 3 * n_query
    qaux_ref[used : used + 1, :] = soft * (math.sqrt(2.0 / (9.0 * n_query)) / 2.0)
    qaux_ref[used + 1 : used + 2, :] = bonus
    qaux_ref[used + 2 : used + 3, :] = wide[96:97, :]
    qaux_ref[used + 3 : used + 4, :] = wide[97:98, :]

    points[...] = jnp.zeros_like(points)
    points[0:12, :] = frames_ref[...]
    columns = points[...].T
    to_rows = (iota((HALF, rows), 0) // SLOTS == iota((HALF, rows), 1)).astype(F32)
    frows_ref[...] = dot(to_rows, columns, HIGH)


def bias_kernel(heads, pair_ref, wb_hbm, bias_ref, here_ref, weights, wb_ref, sem):
    queries = pair_ref.shape[0]
    width = pair_ref.shape[3]
    keys = pair_ref.shape[1] * pair_ref.shape[2]
    each_step = queries // BIAS_STEPS
    copies = []
    for k in range(BIAS_STEPS):
        part = pl.ds(k * each_step, each_step)
        copies.append(pltpu.make_async_copy(pair_ref.at[part], here_ref.at[part], sem.at[k]))
        copies[k].start()
    small = pltpu.make_async_copy(wb_hbm, wb_ref, sem.at[BIAS_STEPS])
    small.start()
    lane = iota((width, HALF), 1)
    row = iota((HALF, width), 0)
    small.wait()
    wb = wb_ref[...].astype(F32)
    each = jnp.zeros((HALF, width), F32)
    for h in range(heads):
        each = jnp.where(row % SLOTS == h, wb[h : h + 1, :], each)
    each = each.T
    for i in range(queries):
        weights[i * width : (i + 1) * width, :] = jnp.where(
            lane // SLOTS == i, each, 0.0
        ).astype(BF16)
    for k in range(BIAS_STEPS):
        copies[k].wait()
        these = range(k * each_step, (k + 1) * each_step)
        left = jnp.concatenate([here_ref[i].reshape(keys, width) for i in these], axis=1)
        found = dot(left, weights[these[0] * width : (these[-1] + 1) * width, :])
        bias_ref[...] = found if k == 0 else bias_ref[...] + found


def attend_kernel(
    n_query, mine_ref, across_ref, bias_ref, qb_ref, qaux_ref, pair_ref, part_ref, turned_w, block
):
    far, half, lanes = mine_ref.shape
    keys = 2 * far * half
    queries = pair_ref.shape[0]
    width = pair_ref.shape[3]
    place = lax.axis_index("near")
    for k in range(far):
        start = pl.multiple_of((2 * k + place) * half, half)
        block[pl.ds(start, half), :] = mine_ref[k]
        start = pl.multiple_of((2 * k + 1 - place) * half, half)
        block[pl.ds(start, half), :] = across_ref[k]
    high = block[:, HALF:]
    first = high.astype(BF16)
    rest = high - first.astype(F32)
    second = rest.astype(BF16)
    third = (rest - second.astype(F32)).astype(BF16)
    split = jnp.concatenate([first, second, third], axis=1)

    row = iota((HALF, HALF), 0)
    lane = iota((HALF, HALF), 1)
    slot = lane % SLOTS

    def expanded(wanted):
        picks = (row == wanted).astype(F32).astype(BF16)
        return dot(split, jnp.concatenate([picks, picks, picks], axis=0))

    distance = jnp.zeros((keys, HALF), F32)
    for a in range(3):
        for p in range(n_query):
            wanted = jnp.where(slot < 3, COMP * a + 12 * slot + p, -1)
            at = n_query * a + p
            gap = qaux_ref[at : at + 1, :] - expanded(wanted)
            distance += gap * gap
    used = 3 * n_query
    scale = qaux_ref[used : used + 1, :]
    bonus = qaux_ref[used + 1 : used + 2, :]
    differ = expanded(jnp.full((HALF, HALF), CHAIN)) != qaux_ref[used + 2 : used + 3, :]
    there = expanded(jnp.full((HALF, HALF), PRESENT)) * qaux_ref[used + 3 : used + 4, :]
    logits = dot(block[:, :HALF], qb_ref[...], HIGH) + LOGIT_WEIGHT * (
        bias_ref[...] - scale * distance + jnp.where(differ, bonus, 0.0)
    )
    logits = logits - MASK_PENALTY * (1.0 - there)
    by_row = logits.T
    top = jnp.max(by_row, axis=1, keepdims=True)
    weights = jnp.exp(by_row - top)
    turned_w[...] = weights
    sums = dot(weights, block[...], HIGH)
    part_ref[:, HALF:] = jnp.where(iota((HALF, lanes), 1) == HALF + TOP, top, sums)
    upper = iota((2 * SLOTS, width), 0) < SLOTS
    for g in range(queries // 2):
        rows = slice(2 * SLOTS * g, 2 * SLOTS * (g + 1))
        right = jnp.concatenate(
            [pair_ref[2 * g].reshape(keys, width), pair_ref[2 * g + 1].reshape(keys, width)],
            axis=1,
        )
        both = dot(turned_w[rows, :].astype(BF16), right)
        part_ref[rows, 0:width] = jnp.where(upper, both[:, :width], both[:, width:])


def merge_kernel(
    heads,
    size,
    n_query,
    n_value,
    mine_ref,
    theirs_ref,
    frows_ref,
    w_out_ref,
    out_ref,
    small,
    large,
):
    copies, rows, _ = out_ref.shape
    tops = [ref[:, 2 * HALF + TOP : 2 * HALF + TOP + 1] for ref in (mine_ref, theirs_ref)]
    sums = [ref[:, 2 * HALF + ONE : 2 * HALF + ONE + 1] for ref in (mine_ref, theirs_ref)]
    best = jnp.maximum(tops[0], tops[1])
    factors = [jnp.exp(top - best) for top in tops]
    total = factors[0] * sums[0] + factors[1] * sums[1]
    merged = (mine_ref[...] * factors[0] + theirs_ref[...] * factors[1]) / total
    slot = iota((HALF, 1), 0) % SLOTS

    def of_own_head(first, step, count):
        picked = jnp.zeros((HALF, count), F32)
        for h in range(heads):
            at = first + step * h
            picked = jnp.where(slot == h, merged[:, at : at + count], picked)
        return picked

    attended = of_own_head(HALF + size, 2 * size, size)
    n_points = n_query + n_value
    moved = [
        of_own_head(2 * HALF + COMP * a + n_query, n_points, n_value)
        - frows_ref[:, 9 + a : 10 + a]
        for a in range(3)
    ]
    pointed = []
    for b in range(3):
        total_b = frows_ref[:, b : b + 1] * moved[0]
        for a in (1, 2):
            total_b += frows_ref[:, 3 * a + b : 3 * a + b + 1] * moved[a]
        pointed.append(total_b)
    norms = jnp.sqrt(
        pointed[0] * pointed[0] + pointed[1] * pointed[1] + pointed[2] * pointed[2] + 1.0
    )
    small[...] = jnp.zeros_like(small)
    small[:, 0:size] = attended
    for b in range(3):
        small[:, size + n_value * b : size + n_value * (b + 1)] = pointed[b]
    edge = size + 3 * n_value
    small[:, edge : edge + n_value] = norms
    source = iota((HALF, HALF), 0)
    target = iota((HALF, HALF), 1)
    inside = (source >= size) & (source < edge)
    goes = jnp.where(
        inside, size + 3 * ((source - size) % n_value) + (source - size) // n_value, source
    )
    order = (goes == target).astype(F32).astype(BF16)
    small[...] = dot(small[...].astype(BF16), order)
    large[...] = merged[:, :HALF]
    cut = edge + n_value
    update = jnp.zeros((rows, w_out_ref.shape[2]), F32)
    for h in range(heads):
        low = small[pl.ds(h, rows, stride=SLOTS), :].astype(BF16)
        update += dot(low[:, :cut], w_out_ref[h, 0:cut, :])
        wide = large[pl.ds(h, rows, stride=SLOTS), :].astype(BF16)
        update += dot(wide, w_out_ref[h, cut:, :])
    for k in range(copies):
        out_ref[k] = update


def finish_kernel(updates_ref, single_ref, gain_ref, wb_ref, frames_ref, out_ref, send_ref):
    copies, rows, channels = updates_ref.shape
    mixed = single_ref[...].astype(F32)
    update = updates_ref[0]
    for k in range(1, copies):
        update += updates_ref[k]
    mixed = mixed + update
    centre = jnp.mean(mixed, axis=1, keepdims=True)
    away = mixed - centre
    spread = jnp.mean(away * away, axis=1, keepdims=True)
    gain = gain_ref[...].reshape(1, channels)
    single_out = (away * lax.rsqrt(spread + 1e-05) * gain).astype(BF16)
    out_ref[...] = single_out
    motion = dot_nt(wb_ref[...], single_out)
    m = [motion[k : k + 1, :] for k in range(6)]
    qa = 1.0 / jnp.sqrt(1.0 + m[0] * m[0] + m[1] * m[1] + m[2] * m[2])
    qb, qc, qd = m[0] * qa, m[1] * qa, m[2] * qa
    spin = [
        [qa * qa + qb * qb - qc * qc - qd * qd, 2.0 * (qb * qc - qa * qd), 2.0 * (qb * qd + qa * qc)],
        [2.0 * (qb * qc + qa * qd), qa * qa - qb * qb + qc * qc - qd * qd, 2.0 * (qc * qd - qa * qb)],
        [2.0 * (qb * qd - qa * qc), 2.0 * (qc * qd + qa * qb), qa * qa - qb * qb - qc * qc + qd * qd],
    ]
    r = [[frames_ref[3 * a + b : 3 * a + b + 1, :] for b in range(3)] for a in range(3)]
    lines = []
    for a in range(3):
        for c in range(3):
            lines.append(r[a][0] * spin[0][c] + r[a][1] * spin[1][c] + r[a][2] * spin[2][c])
    for a in range(3):
        lines.append(
            frames_ref[9 + a : 10 + a, :] + (r[a][0] * m[3] + r[a][1] * m[4] + r[a][2] * m[5])
        )
    groups = HALF // rows
    repeat = (iota((rows, HALF), 1) % rows == iota((rows, HALF), 0)).astype(F32)
    wide = dot(jnp.concatenate(lines + lines[:4], axis=0), repeat, HIGH)
    group = iota((1, HALF), 1) // rows
    pieces = []
    for v in range(len(lines) // groups):
        piece = wide[groups * v : groups * v + 1, :]
        for s in range(1, groups):
            at = groups * v + s
            piece = jnp.where(group == s, wide[at : at + 1, :], piece)
        pieces.append(piece)
    line = jnp.concatenate(pieces, axis=1)
    send_ref[...] = jnp.broadcast_to(line, (send_ref.shape[0], line.shape[1])).reshape(
        send_ref.shape
    )


def spread_kernel(blocks_ref, out_ref):
    blocks, _, wide = blocks_ref.shape
    lines = out_ref.shape[0]
    rows = wide // lines
    groups = HALF // rows
    x = blocks_ref[...].reshape(blocks, wide)
    s = iota((blocks, HALF), 0) % groups
    g = iota((blocks, HALF), 1) // rows
    for v in range(wide // HALF):
        tile = x[:, HALF * v : HALF * (v + 1)]
        z = tile
        for d in range(1, groups):
            right = pltpu.roll(tile, rows * d, 1)
            up = pltpu.roll(right, blocks - d, 0)
            down = pltpu.roll(right, groups - d, 0)
            z = jnp.where(g - s == d, up, z)
            z = jnp.where(g - s == d - groups, down, z)
        for q in range(blocks // groups):
            out_ref[groups * v : groups * (v + 1), HALF * q : HALF * (q + 1)] = z[
                groups * q : groups * (q + 1), :
            ]


def in_hbm(x):
    return pltpu.with_memory_space_constraint(x, pltpu.HBM)


def call(kernel, outs, scratch=(), specs=None, n=0, room=4, cost=None, name=None):
    return pl.pallas_call(
        kernel,
        out_shape=outs,
        in_specs=specs or [VMEM] * n,
        out_specs=jax.tree.map(lambda _: VMEM, outs),
        scratch_shapes=list(scratch),
        cost_estimate=cost,
        compiler_params=pltpu.CompilerParams(vmem_limit_bytes=room * 1024 * 1024),
        name=name,
    )


def body(
    single,
    pair,
    frames,
    chain,
    mask,
    w_query,
    w_key_value,
    w_query_points,
    w_kv_points,
    w_pair_bias,
    head_weights,
    chain_bias,
    w_out,
    out_gain,
    w_backbone,
):
    rows, channels = single.shape
    blocks, half = pair.shape[1], pair.shape[2]
    width = pair.shape[3]
    heads = w_pair_bias.shape[1]
    size = w_query.shape[1] // heads
    n_query = w_query_points.shape[1] // (3 * heads)
    n_points = w_kv_points.shape[1] // (3 * heads)
    n_value = n_points - n_query
    keys = blocks * half
    shape = jax.ShapeDtypeStruct

    inputs = (
        single,
        frames,
        chain,
        mask,
        w_query.T,
        w_key_value.T,
        w_query_points.T,
        w_kv_points.T,
        head_weights,
        chain_bias,
    )
    payload, qb, qaux, frows = call(
        functools.partial(project_kernel, heads, size, n_query, n_points),
        (
            shape((half, 2 * HALF), F32),
            shape((HALF, HALF), F32),
            shape((16, HALF), F32),
            shape((HALF, HALF), F32),
        ),
        (
            pltpu.VMEM((3 * HALF, rows), F32),
            pltpu.VMEM((HALF, rows), F32),
            pltpu.VMEM((rows, 2 * HALF), F32),
            pltpu.VMEM((104, rows), F32),
            *(pltpu.VMEM(x.shape, x.dtype) for x in inputs[:8]),
            *(pltpu.SMEM(x.shape, x.dtype) for x in inputs[8:]),
            pltpu.SemaphoreType.DMA((len(inputs),)),
        ),
        specs=[HBM] * len(inputs),
        name="project",
    )(*(in_hbm(x) for x in inputs))
    gathered = lax.all_gather(payload, "far", axis=0, tiled=False)
    swap = [(k, 1 - k) for k in range(2)]
    across = lax.ppermute(gathered, "near", swap)
    bias, pair_here = call(
        functools.partial(bias_kernel, heads),
        (shape((keys, HALF), F32), shape(pair.shape, pair.dtype)),
        (
            pltpu.VMEM((rows * width, HALF), BF16),
            pltpu.VMEM((heads, width), w_pair_bias.dtype),
            pltpu.SemaphoreType.DMA((BIAS_STEPS + 1,)),
        ),
        specs=[HBM, HBM],
        room=16,
        cost=pl.CostEstimate(flops=10**9, bytes_accessed=2 * pair.size, transcendentals=0),
        name="bias",
    )(in_hbm(pair), in_hbm(w_pair_bias.T))
    part = call(
        functools.partial(attend_kernel, n_query),
        shape((HALF, 3 * HALF), F32),
        (pltpu.VMEM((HALF, keys), F32), pltpu.VMEM((keys, 2 * HALF), F32)),
        n=6,
        room=24,
        name="attend",
    )(gathered, across, bias, qb, qaux, pair_here)
    other = lax.ppermute(part, "pair", swap)
    updates = call(
        functools.partial(merge_kernel, heads, size, n_query, n_value),
        shape((lax.axis_size("head"), rows, channels), F32),
        (pltpu.VMEM((HALF, HALF), F32), pltpu.VMEM((HALF, HALF), F32)),
        n=4,
        name="merge",
    )(part, other, frows, w_out)
    updates = lax.all_to_all(updates, "head", split_axis=0, concat_axis=0, tiled=True)
    single_out, send = call(
        finish_kernel,
        (shape((rows, channels), BF16), shape((blocks, 1, 12 * rows), F32)),
        n=5,
        name="finish",
    )(updates, single, out_gain, w_backbone.T, frames)
    received = lax.all_to_all(send, ("far", "near"), split_axis=0, concat_axis=0, tiled=True)
    frames_out = call(
        spread_kernel, shape((12, blocks * rows), F32), n=1, name="spread"
    )(received)
    return (single_out, frames_out)


def solution(mesh):
    groups, blocks, heads, pairs = (mesh.shape[a] for a in ("groups", "blk", "head", "pair"))
    near = 2
    finer = Mesh(
        mesh.devices.reshape(groups, blocks // near, near, heads, pairs),
        ("groups", "far", "near", "head", "pair"),
    )
    split = ("groups", "far", "near")
    placed = (
        P(split, None),
        P(split, None, "pair", None),
        P(None, split),
        P(split),
        P(split),
        P(None, "head"),
        P(None, "head"),
        P(None, "head"),
        P(None, "head"),
        P(None, "head"),
        P("head"),
        P("head"),
        P("head", None, None),
        P(),
        P(),
    )
    return jax.shard_map(
        body,
        mesh=finer,
        in_specs=placed,
        out_specs=(P(split, None), P(None, "groups")),
        check_vma=False,
    )
```

```python
import functools
import math

import jax
import jax.numpy as jnp
from jax import lax
from jax.experimental import pallas as pl
from jax.experimental.pallas import tpu as pltpu
from jax.sharding import PartitionSpec as P

HIGH = lax.Precision.HIGHEST
LOGIT_WEIGHT = math.sqrt(1.0 / 3.0)
MASK_PENALTY = 100000.0
F32 = jnp.float32
BF16 = jnp.bfloat16

SLOTS = 4
HALF = 128
BIAS_STEPS = 4
COMP = 40
CHAIN, PRESENT, ONE, TOP = 120, 121, 122, 123
VMEM = pl.BlockSpec(memory_space=pltpu.VMEM)
HBM = pl.BlockSpec(memory_space=pltpu.HBM)


def iota(shape, dim):
    return lax.broadcasted_iota(jnp.int32, shape, dim)


def dot(a, b, precision=None):
    return jnp.dot(a, b, preferred_element_type=F32, precision=precision)


def dot_nt(a, b):
    return lax.dot_general(a, b, (((1,), (1,)), ((), ())), preferred_element_type=F32)


def rotated(frames_ref, parts):
    moved = []
    for a in range(3):
        total = frames_ref[3 * a : 3 * a + 1, :] * parts[0]
        for b in (1, 2):
            total += frames_ref[3 * a + b : 3 * a + b + 1, :] * parts[b]
        moved.append(total + frames_ref[9 + a : 10 + a, :])
    return moved


def project_kernel(
    heads,
    size,
    n_query,
    n_points,
    *refs,
):
    sources, refs = refs[:10], refs[10:]
    payload_ref, qb_ref, qaux_ref, frows_ref, turned, points, full, spread = refs[:8]
    local_refs, sem = refs[8:18], refs[18]
    copies = [
        pltpu.make_async_copy(source, target, sem.at[k])
        for k, (source, target) in enumerate(zip(sources, local_refs))
    ]
    for copy in copies:
        copy.start()
    single_ref, frames_ref, chain_ref, mask_ref, wq_ref, wkv_ref, wqp_ref, wkp_ref = local_refs[:8]
    hw_ref, cb_ref = local_refs[8:]
    full[...] = jnp.zeros_like(full)
    points[...] = jnp.zeros_like(points)
    spread[...] = jnp.zeros_like(spread)
    qb_ref[...] = jnp.zeros_like(qb_ref)
    qaux_ref[...] = jnp.zeros_like(qaux_ref)
    for copy in copies:
        copy.wait()
    rows = single_ref.shape[0]
    half = payload_ref.shape[0]
    x = single_ref[...]
    q_wide = heads * size
    turned[HALF : HALF + 3 * heads * n_query, :] = dot_nt(wqp_ref[...], x)
    turned[2 * HALF : 2 * HALF + 3 * heads * n_points, :] = dot_nt(wkp_ref[...], x)
    full[:, 0 : 2 * q_wide] = dot_nt(x, wkv_ref[...])
    chain_row = chain_ref[...].astype(F32).reshape(1, rows)
    mask_row = mask_ref[...].astype(F32).reshape(1, rows)

    count = heads * n_points
    local = [turned[pl.ds(2 * HALF + b, count, stride=3), :] for b in range(3)]
    for a, value in enumerate(rotated(frames_ref, local)):
        points[COMP * a : COMP * a + count, :] = value
    points[CHAIN : CHAIN + 1, :] = chain_row
    points[PRESENT : PRESENT + 1, :] = mask_row
    points[ONE : ONE + 1, :] = jnp.ones((1, rows), F32)
    full[:, HALF:] = points[...].T
    start = pl.multiple_of(lax.axis_index("pair") * half, half)
    payload_ref[...] = full[pl.ds(start, half), :]

    count = heads * n_query
    local = [turned[pl.ds(HALF + b, count, stride=3), :] for b in range(3)]
    spread[0:q_wide, :] = dot_nt(wq_ref[...], x)
    for a, value in enumerate(rotated(frames_ref, local)):
        spread[48 + 16 * a : 48 + 16 * a + count, :] = value
    spread[96:97, :] = chain_row
    spread[97:98, :] = mask_row
    to_slots = (iota((rows, HALF), 1) // SLOTS == iota((rows, HALF), 0)).astype(F32)
    wide = dot(spread[...], to_slots, HIGH)
    slot = iota((1, HALF), 1) % SLOTS
    scale = LOGIT_WEIGHT / math.sqrt(size)
    for h in range(heads):
        block = wide[h * size : (h + 1) * size, :] * scale
        qb_ref[2 * size * h : 2 * size * h + size, :] = jnp.where(slot == h, block, 0.0)
    for a in range(3):
        for p in range(n_query):
            line = jnp.zeros((1, HALF), F32)
            for h in range(heads):
                at = 48 + 16 * a + h * n_query + p
                line = jnp.where(slot == h, wide[at : at + 1, :], line)
            qaux_ref[n_query * a + p : n_query * a + p + 1, :] = line
    raw = jnp.zeros((1, HALF), F32)
    bonus = jnp.zeros((1, HALF), F32)
    for h in range(heads):
        raw = jnp.where(slot == h, hw_ref[h], raw)
        bonus = jnp.where(slot == h, cb_ref[h], bonus)
    soft = jnp.maximum(raw, 0.0) + jnp.log1p(jnp.exp(-jnp.abs(raw)))
    used = 3 * n_query
    qaux_ref[used : used + 1, :] = soft * (math.sqrt(2.0 / (9.0 * n_query)) / 2.0)
    qaux_ref[used + 1 : used + 2, :] = bonus
    qaux_ref[used + 2 : used + 3, :] = wide[96:97, :]
    qaux_ref[used + 3 : used + 4, :] = wide[97:98, :]

    points[...] = jnp.zeros_like(points)
    points[0:12, :] = frames_ref[...]
    columns = points[...].T
    to_rows = (iota((HALF, rows), 0) // SLOTS == iota((HALF, rows), 1)).astype(F32)
    frows_ref[...] = dot(to_rows, columns, HIGH)


def bias_kernel(heads, pair_ref, wb_hbm, bias_ref, here_ref, weights, wb_ref, sem):
    queries = pair_ref.shape[0]
    width = pair_ref.shape[3]
    keys = pair_ref.shape[1] * pair_ref.shape[2]
    each_step = queries // BIAS_STEPS
    copies = []
    for k in range(BIAS_STEPS):
        part = pl.ds(k * each_step, each_step)
        copies.append(pltpu.make_async_copy(pair_ref.at[part], here_ref.at[part], sem.at[k]))
        copies[k].start()
    small = pltpu.make_async_copy(wb_hbm, wb_ref, sem.at[BIAS_STEPS])
    small.start()
    lane = iota((width, HALF), 1)
    row = iota((HALF, width), 0)
    small.wait()
    wb = wb_ref[...].astype(F32)
    each = jnp.zeros((HALF, width), F32)
    for h in range(heads):
        each = jnp.where(row % SLOTS == h, wb[h : h + 1, :], each)
    each = each.T
    for i in range(queries):
        weights[i * width : (i + 1) * width, :] = jnp.where(
            lane // SLOTS == i, each, 0.0
        ).astype(BF16)
    for k in range(BIAS_STEPS):
        copies[k].wait()
        these = range(k * each_step, (k + 1) * each_step)
        left = jnp.concatenate([here_ref[i].reshape(keys, width) for i in these], axis=1)
        found = dot(left, weights[these[0] * width : (these[-1] + 1) * width, :])
        bias_ref[...] = found if k == 0 else bias_ref[...] + found


def attend_kernel(
    n_query, mine_ref, across_ref, bias_ref, qb_ref, qaux_ref, pair_ref, part_ref, turned_w, block
):
    far, half, lanes = mine_ref.shape
    keys = 2 * far * half
    queries = pair_ref.shape[0]
    width = pair_ref.shape[3]
    place = lax.axis_index("blk") % 2
    for k in range(far):
        start = pl.multiple_of((2 * k + place) * half, half)
        block[pl.ds(start, half), :] = mine_ref[k]
        start = pl.multiple_of((2 * k + 1 - place) * half, half)
        block[pl.ds(start, half), :] = across_ref[k]
    high = block[:, HALF:]
    first = high.astype(BF16)
    rest = high - first.astype(F32)
    second = rest.astype(BF16)
    third = (rest - second.astype(F32)).astype(BF16)
    split = jnp.concatenate([first, second, third], axis=1)

    row = iota((HALF, HALF), 0)
    lane = iota((HALF, HALF), 1)
    slot = lane % SLOTS

    def expanded(wanted):
        picks = (row == wanted).astype(F32).astype(BF16)
        return dot(split, jnp.concatenate([picks, picks, picks], axis=0))

    distance = jnp.zeros((keys, HALF), F32)
    for a in range(3):
        for p in range(n_query):
            wanted = jnp.where(slot < 3, COMP * a + 12 * slot + p, -1)
            at = n_query * a + p
            gap = qaux_ref[at : at + 1, :] - expanded(wanted)
            distance += gap * gap
    used = 3 * n_query
    scale = qaux_ref[used : used + 1, :]
    bonus = qaux_ref[used + 1 : used + 2, :]
    differ = expanded(jnp.full((HALF, HALF), CHAIN)) != qaux_ref[used + 2 : used + 3, :]
    there = expanded(jnp.full((HALF, HALF), PRESENT)) * qaux_ref[used + 3 : used + 4, :]
    logits = dot(block[:, :HALF], qb_ref[...], HIGH) + LOGIT_WEIGHT * (
        bias_ref[...] - scale * distance + jnp.where(differ, bonus, 0.0)
    )
    logits = logits - MASK_PENALTY * (1.0 - there)
    by_row = logits.T
    top = jnp.max(by_row, axis=1, keepdims=True)
    weights = jnp.exp(by_row - top)
    turned_w[...] = weights
    sums = dot(weights, block[...], HIGH)
    part_ref[:, HALF:] = jnp.where(iota((HALF, lanes), 1) == HALF + TOP, top, sums)
    upper = iota((2 * SLOTS, width), 0) < SLOTS
    for g in range(queries // 2):
        rows = slice(2 * SLOTS * g, 2 * SLOTS * (g + 1))
        right = jnp.concatenate(
            [pair_ref[2 * g].reshape(keys, width), pair_ref[2 * g + 1].reshape(keys, width)],
            axis=1,
        )
        both = dot(turned_w[rows, :].astype(BF16), right)
        part_ref[rows, 0:width] = jnp.where(upper, both[:, :width], both[:, width:])


def merge_kernel(
    heads,
    size,
    n_query,
    n_value,
    mine_ref,
    theirs_ref,
    frows_ref,
    w_out_ref,
    out_ref,
    small,
    large,
):
    copies, rows, _ = out_ref.shape
    tops = [ref[:, 2 * HALF + TOP : 2 * HALF + TOP + 1] for ref in (mine_ref, theirs_ref)]
    sums = [ref[:, 2 * HALF + ONE : 2 * HALF + ONE + 1] for ref in (mine_ref, theirs_ref)]
    best = jnp.maximum(tops[0], tops[1])
    factors = [jnp.exp(top - best) for top in tops]
    total = factors[0] * sums[0] + factors[1] * sums[1]
    merged = (mine_ref[...] * factors[0] + theirs_ref[...] * factors[1]) / total
    slot = iota((HALF, 1), 0) % SLOTS

    def of_own_head(first, step, count):
        picked = jnp.zeros((HALF, count), F32)
        for h in range(heads):
            at = first + step * h
            picked = jnp.where(slot == h, merged[:, at : at + count], picked)
        return picked

    attended = of_own_head(HALF + size, 2 * size, size)
    n_points = n_query + n_value
    moved = [
        of_own_head(2 * HALF + COMP * a + n_query, n_points, n_value)
        - frows_ref[:, 9 + a : 10 + a]
        for a in range(3)
    ]
    pointed = []
    for b in range(3):
        total_b = frows_ref[:, b : b + 1] * moved[0]
        for a in (1, 2):
            total_b += frows_ref[:, 3 * a + b : 3 * a + b + 1] * moved[a]
        pointed.append(total_b)
    norms = jnp.sqrt(
        pointed[0] * pointed[0] + pointed[1] * pointed[1] + pointed[2] * pointed[2] + 1.0
    )
    small[...] = jnp.zeros_like(small)
    small[:, 0:size] = attended
    for b in range(3):
        small[:, size + n_value * b : size + n_value * (b + 1)] = pointed[b]
    edge = size + 3 * n_value
    small[:, edge : edge + n_value] = norms
    source = iota((HALF, HALF), 0)
    target = iota((HALF, HALF), 1)
    inside = (source >= size) & (source < edge)
    goes = jnp.where(
        inside, size + 3 * ((source - size) % n_value) + (source - size) // n_value, source
    )
    order = (goes == target).astype(F32).astype(BF16)
    small[...] = dot(small[...].astype(BF16), order)
    large[...] = merged[:, :HALF]
    cut = edge + n_value
    update = jnp.zeros((rows, w_out_ref.shape[2]), F32)
    for h in range(heads):
        low = small[pl.ds(h, rows, stride=SLOTS), :].astype(BF16)
        update += dot(low[:, :cut], w_out_ref[h, 0:cut, :])
        wide = large[pl.ds(h, rows, stride=SLOTS), :].astype(BF16)
        update += dot(wide, w_out_ref[h, cut:, :])
    for k in range(copies):
        out_ref[k] = update


def finish_kernel(updates_ref, single_ref, gain_ref, wb_ref, frames_ref, out_ref, send_ref):
    copies, rows, channels = updates_ref.shape
    mixed = single_ref[...].astype(F32)
    update = updates_ref[0]
    for k in range(1, copies):
        update += updates_ref[k]
    mixed = mixed + update
    centre = jnp.mean(mixed, axis=1, keepdims=True)
    away = mixed - centre
    spread = jnp.mean(away * away, axis=1, keepdims=True)
    gain = gain_ref[...].reshape(1, channels)
    single_out = (away * lax.rsqrt(spread + 1e-05) * gain).astype(BF16)
    out_ref[...] = single_out
    motion = dot_nt(wb_ref[...], single_out)
    m = [motion[k : k + 1, :] for k in range(6)]
    qa = 1.0 / jnp.sqrt(1.0 + m[0] * m[0] + m[1] * m[1] + m[2] * m[2])
    qb, qc, qd = m[0] * qa, m[1] * qa, m[2] * qa
    spin = [
        [qa * qa + qb * qb - qc * qc - qd * qd, 2.0 * (qb * qc - qa * qd), 2.0 * (qb * qd + qa * qc)],
        [2.0 * (qb * qc + qa * qd), qa * qa - qb * qb + qc * qc - qd * qd, 2.0 * (qc * qd - qa * qb)],
        [2.0 * (qb * qd - qa * qc), 2.0 * (qc * qd + qa * qb), qa * qa - qb * qb - qc * qc + qd * qd],
    ]
    r = [[frames_ref[3 * a + b : 3 * a + b + 1, :] for b in range(3)] for a in range(3)]
    lines = []
    for a in range(3):
        for c in range(3):
            lines.append(r[a][0] * spin[0][c] + r[a][1] * spin[1][c] + r[a][2] * spin[2][c])
    for a in range(3):
        lines.append(
            frames_ref[9 + a : 10 + a, :] + (r[a][0] * m[3] + r[a][1] * m[4] + r[a][2] * m[5])
        )
    groups = HALF // rows
    repeat = (iota((rows, HALF), 1) % rows == iota((rows, HALF), 0)).astype(F32)
    wide = dot(jnp.concatenate(lines + lines[:4], axis=0), repeat, HIGH)
    group = iota((1, HALF), 1) // rows
    pieces = []
    for v in range(len(lines) // groups):
        piece = wide[groups * v : groups * v + 1, :]
        for s in range(1, groups):
            at = groups * v + s
            piece = jnp.where(group == s, wide[at : at + 1, :], piece)
        pieces.append(piece)
    line = jnp.concatenate(pieces, axis=1)
    send_ref[...] = jnp.broadcast_to(line, (send_ref.shape[0], line.shape[1])).reshape(
        send_ref.shape
    )


def spread_kernel(first, blocks_ref, out_ref):
    blocks, _, wide = blocks_ref.shape
    lines = out_ref.shape[0]
    rows = wide // lines
    groups = HALF // rows
    x = blocks_ref[...].reshape(blocks, wide)
    s = iota((blocks, HALF), 0) % groups
    g = iota((blocks, HALF), 1) // rows
    for v in range(wide // HALF):
        tile = x[:, HALF * v : HALF * (v + 1)]
        z = tile
        for d in range(1, groups):
            right = pltpu.roll(tile, rows * d, 1)
            up = pltpu.roll(right, blocks - d, 0)
            down = pltpu.roll(right, groups - d, 0)
            z = jnp.where(g - s == d, up, z)
            z = jnp.where(g - s == d - groups, down, z)
        for q in range(blocks // groups):
            at = (HALF * q + rows * first) % (rows * blocks)
            out_ref[groups * v : groups * (v + 1), at : at + HALF] = z[
                groups * q : groups * (q + 1), :
            ]


def in_hbm(x):
    return pltpu.with_memory_space_constraint(x, pltpu.HBM)


def call(kernel, outs, scratch=(), specs=None, n=0, room=4, cost=None, name=None):
    return pl.pallas_call(
        kernel,
        out_shape=outs,
        in_specs=specs or [VMEM] * n,
        out_specs=jax.tree.map(lambda _: VMEM, outs),
        scratch_shapes=list(scratch),
        cost_estimate=cost,
        compiler_params=pltpu.CompilerParams(vmem_limit_bytes=room * 1024 * 1024),
        name=name,
    )


def body(
    single,
    pair,
    frames,
    chain,
    mask,
    w_query,
    w_key_value,
    w_query_points,
    w_kv_points,
    w_pair_bias,
    head_weights,
    chain_bias,
    w_out,
    out_gain,
    w_backbone,
):
    rows, channels = single.shape
    blocks, half = pair.shape[1], pair.shape[2]
    width = pair.shape[3]
    heads = w_pair_bias.shape[1]
    size = w_query.shape[1] // heads
    n_query = w_query_points.shape[1] // (3 * heads)
    n_points = w_kv_points.shape[1] // (3 * heads)
    n_value = n_points - n_query
    keys = blocks * half
    shape = jax.ShapeDtypeStruct

    inputs = (
        single,
        frames,
        chain,
        mask,
        w_query.T,
        w_key_value.T,
        w_query_points.T,
        w_kv_points.T,
        head_weights,
        chain_bias,
    )
    payload, qb, qaux, frows = call(
        functools.partial(project_kernel, heads, size, n_query, n_points),
        (
            shape((half, 2 * HALF), F32),
            shape((HALF, HALF), F32),
            shape((16, HALF), F32),
            shape((HALF, HALF), F32),
        ),
        (
            pltpu.VMEM((3 * HALF, rows), F32),
            pltpu.VMEM((HALF, rows), F32),
            pltpu.VMEM((rows, 2 * HALF), F32),
            pltpu.VMEM((104, rows), F32),
            *(pltpu.VMEM(x.shape, x.dtype) for x in inputs[:8]),
            *(pltpu.SMEM(x.shape, x.dtype) for x in inputs[8:]),
            pltpu.SemaphoreType.DMA((len(inputs),)),
        ),
        specs=[HBM] * len(inputs),
        name="project",
    )(*(in_hbm(x) for x in inputs))
    ways = [list(range(k, blocks, 2)) for k in range(2)]
    gathered = lax.all_gather(payload, "blk", axis=0, axis_index_groups=ways, tiled=False)
    swap = [(k, k + 1 - 2 * (k % 2)) for k in range(blocks)]
    across = lax.ppermute(gathered, "blk", swap)
    bias, pair_here = call(
        functools.partial(bias_kernel, heads),
        (shape((keys, HALF), F32), shape(pair.shape, pair.dtype)),
        (
            pltpu.VMEM((rows * width, HALF), BF16),
            pltpu.VMEM((heads, width), w_pair_bias.dtype),
            pltpu.SemaphoreType.DMA((BIAS_STEPS + 1,)),
        ),
        specs=[HBM, HBM],
        room=16,
        cost=pl.CostEstimate(flops=10**9, bytes_accessed=2 * pair.size, transcendentals=0),
        name="bias",
    )(in_hbm(pair), in_hbm(w_pair_bias.T))
    part = call(
        functools.partial(attend_kernel, n_query),
        shape((HALF, 3 * HALF), F32),
        (pltpu.VMEM((HALF, keys), F32), pltpu.VMEM((keys, 2 * HALF), F32)),
        n=6,
        room=24,
        name="attend",
    )(gathered, across, bias, qb, qaux, pair_here)
    other = lax.ppermute(part, "pair", [(0, 1), (1, 0)])
    updates = call(
        functools.partial(merge_kernel, heads, size, n_query, n_value),
        shape((lax.axis_size("head"), rows, channels), F32),
        (pltpu.VMEM((HALF, HALF), F32), pltpu.VMEM((HALF, HALF), F32)),
        n=4,
        name="merge",
    )(part, other, frows, w_out)
    updates = lax.all_to_all(updates, "head", split_axis=0, concat_axis=0, tiled=True)
    single_out, send = call(
        finish_kernel,
        (shape((rows, channels), BF16), shape((blocks, 1, 12 * rows), F32)),
        n=5,
        name="finish",
    )(updates, single, out_gain, w_backbone.T, frames)
    middle_first = [(k + blocks // 2) % blocks for k in range(blocks)]
    received = lax.all_to_all(
        send, "blk", split_axis=0, concat_axis=0, axis_index_groups=[middle_first], tiled=True
    )
    frames_out = call(
        functools.partial(spread_kernel, middle_first[0]),
        shape((12, blocks * rows), F32),
        n=1,
        name="spread",
    )(received)
    return (single_out, frames_out)


def solution(mesh):
    split = ("groups", "blk")
    placed = (
        P(split, None),
        P(split, None, "pair", None),
        P(None, split),
        P(split),
        P(split),
        P(None, "head"),
        P(None, "head"),
        P(None, "head"),
        P(None, "head"),
        P(None, "head"),
        P("head"),
        P("head"),
        P("head", None, None),
        P(),
        P(),
    )
    return jax.shard_map(
        body,
        mesh=mesh,
        in_specs=placed,
        out_specs=(P(split, None), P(None, "groups")),
        check_vma=False,
    )
```

```python
import functools
import math

import jax
import jax.numpy as jnp
from jax import lax
from jax.experimental import pallas as pl
from jax.experimental.pallas import tpu as pltpu
from jax.sharding import PartitionSpec as P

HIGH = lax.Precision.HIGHEST
LOGIT_WEIGHT = math.sqrt(1.0 / 3.0)
MASK_PENALTY = 100000.0
F32 = jnp.float32
BF16 = jnp.bfloat16

SLOTS = 4
HALF = 128
KEYED = 40
CHAIN, PRESENT, ONE, TOP = 36, 37, 38, 39
VMEM = pl.BlockSpec(memory_space=pltpu.VMEM)
SMEM = pl.BlockSpec(memory_space=pltpu.SMEM)
HBM = pl.BlockSpec(memory_space=pltpu.HBM)


def iota(shape, dim):
    return lax.broadcasted_iota(jnp.int32, shape, dim)


def dot(a, b, precision=None):
    return jnp.dot(a, b, preferred_element_type=F32, precision=precision)


def dot_nt(a, b):
    return lax.dot_general(a, b, (((1,), (1,)), ((), ())), preferred_element_type=F32)


def rotated(frames_ref, parts):
    moved = []
    for a in range(3):
        total = frames_ref[3 * a : 3 * a + 1, :] * parts[0]
        for b in (1, 2):
            total += frames_ref[3 * a + b : 3 * a + b + 1, :] * parts[b]
        moved.append(total + frames_ref[9 + a : 10 + a, :])
    return moved


def keys_kernel(heads, size, n_query, n_points, *refs):
    sources, refs = refs[:6], refs[6:]
    payload_ref, turned, points, full = refs[:4]
    local_refs, sem = refs[4:10], refs[10]
    copies = [
        pltpu.make_async_copy(source, target, sem.at[k])
        for k, (source, target) in enumerate(zip(sources, local_refs))
    ]
    for copy in copies:
        copy.start()
    single_ref, frames_ref, chain_ref, mask_ref, wkv_ref, wkp_ref = local_refs
    full[...] = jnp.zeros_like(full)
    points[...] = jnp.zeros_like(points)
    for copy in copies:
        copy.wait()
    rows = single_ref.shape[0]
    half = payload_ref.shape[0]
    n_value = n_points - n_query
    x = single_ref[...]
    turned[...] = dot_nt(wkp_ref[...], x)
    full[:, 0 : 2 * heads * size] = dot_nt(x, wkv_ref[...])
    count = heads * n_points
    local = [turned[pl.ds(b, count, stride=3), :] for b in range(3)]
    for a, value in enumerate(rotated(frames_ref, local)):
        for h in range(heads):
            at = heads * n_query * a + n_query * h
            points[at : at + n_query, :] = value[n_points * h : n_points * h + n_query, :]
            at = KEYED + heads * n_value * a + n_value * h
            points[at : at + n_value, :] = value[n_points * h + n_query : n_points * (h + 1), :]
    points[CHAIN : CHAIN + 1, :] = chain_ref[...].astype(F32).reshape(1, rows)
    points[PRESENT : PRESENT + 1, :] = mask_ref[...].astype(F32).reshape(1, rows)
    points[ONE : ONE + 1, :] = jnp.ones((1, rows), F32)
    full[:, HALF:] = points[...].T
    start = pl.multiple_of(lax.axis_index("pair") * half, half)
    payload_ref[...] = full[pl.ds(start, half), :]


def queries_kernel(
    heads,
    size,
    n_query,
    single_ref,
    frames_ref,
    chain_ref,
    mask_ref,
    wq_ref,
    wqp_ref,
    hw_ref,
    cb_ref,
    qb_ref,
    qaux_ref,
    frows_ref,
    turned,
    points,
    spread,
):
    rows = single_ref.shape[0]
    x = single_ref[...]
    turned[...] = dot_nt(wqp_ref[...], x)
    count = heads * n_query
    local = [turned[pl.ds(b, count, stride=3), :] for b in range(3)]
    spread[...] = jnp.zeros_like(spread)
    spread[0 : heads * size, :] = dot_nt(wq_ref[...], x)
    for a, value in enumerate(rotated(frames_ref, local)):
        spread[48 + 16 * a : 48 + 16 * a + count, :] = value
    spread[96:97, :] = chain_ref[...].astype(F32).reshape(1, rows)
    spread[97:98, :] = mask_ref[...].astype(F32).reshape(1, rows)
    to_slots = (iota((rows, HALF), 1) // SLOTS == iota((rows, HALF), 0)).astype(F32)
    wide = dot(spread[...], to_slots, HIGH)
    slot = iota((1, HALF), 1) % SLOTS
    qb_ref[...] = jnp.zeros_like(qb_ref)
    scale = LOGIT_WEIGHT / math.sqrt(size)
    for h in range(heads):
        block = wide[h * size : (h + 1) * size, :] * scale
        qb_ref[2 * size * h : 2 * size * h + size, :] = jnp.where(slot == h, block, 0.0)
    qaux_ref[...] = jnp.zeros_like(qaux_ref)
    for a in range(3):
        for p in range(n_query):
            line = jnp.zeros((1, HALF), F32)
            for h in range(heads):
                at = 48 + 16 * a + h * n_query + p
                line = jnp.where(slot == h, wide[at : at + 1, :], line)
            qaux_ref[n_query * a + p : n_query * a + p + 1, :] = line
    raw = jnp.zeros((1, HALF), F32)
    bonus = jnp.zeros((1, HALF), F32)
    for h in range(heads):
        raw = jnp.where(slot == h, hw_ref[h], raw)
        bonus = jnp.where(slot == h, cb_ref[h], bonus)
    soft = jnp.maximum(raw, 0.0) + jnp.log1p(jnp.exp(-jnp.abs(raw)))
    used = 3 * n_query
    qaux_ref[used : used + 1, :] = soft * (math.sqrt(2.0 / (9.0 * n_query)) / 2.0)
    qaux_ref[used + 1 : used + 2, :] = bonus
    qaux_ref[used + 2 : used + 3, :] = wide[96:97, :]
    qaux_ref[used + 3 : used + 4, :] = wide[97:98, :]
    points[...] = jnp.zeros_like(points)
    points[0:12, :] = frames_ref[...]
    to_rows = (iota((HALF, rows), 0) // SLOTS == iota((HALF, rows), 1)).astype(F32)
    frows_ref[...] = dot(to_rows, points[...].T, HIGH)


def scores(n_query, block, qb_ref, qaux_ref):
    keep = iota((block.shape[0], HALF), 1) < KEYED
    high = jnp.where(keep, block[:, HALF:], 0.0)
    first = high.astype(BF16).astype(F32)
    rest = high - first
    second = rest.astype(BF16).astype(F32)
    third = (rest - second).astype(BF16).astype(F32)
    split = first + pltpu.roll(second, KEYED, 1) + pltpu.roll(third, 2 * KEYED, 1)
    split = split.astype(BF16)
    row = iota((HALF, HALF), 0)
    lane = iota((HALF, HALF), 1)
    slot = lane % SLOTS
    heads = CHAIN // (3 * n_query)
    wanted = [
        jnp.where(slot < heads, n_query * (heads * a + slot) + p, -1)
        for a in range(3)
        for p in range(n_query)
    ]
    wanted += [jnp.full((HALF, HALF), CHAIN), jnp.full((HALF, HALF), PRESENT)]
    found = []
    for k in range(0, len(wanted), 2):
        picks = [
            ((row % KEYED == w) & (row < 3 * KEYED)).astype(F32).astype(BF16)
            for w in wanted[k : k + 2]
        ]
        both = dot(split, jnp.concatenate(picks, axis=1))
        found += [both[:, :HALF], both[:, HALF:]]
    used = 3 * n_query
    distance = jnp.zeros((block.shape[0], HALF), F32)
    for k in range(used):
        gap = qaux_ref[k : k + 1, :] - found[k]
        distance += gap * gap
    scale = qaux_ref[used : used + 1, :]
    bonus = qaux_ref[used + 1 : used + 2, :]
    differ = found[used] != qaux_ref[used + 2 : used + 3, :]
    there = found[used + 1] * qaux_ref[used + 3 : used + 4, :]
    partial = dot(block[:, :HALF], qb_ref[...], HIGH) + LOGIT_WEIGHT * (
        jnp.where(differ, bonus, 0.0) - scale * distance
    )
    return partial, MASK_PENALTY * (1.0 - there)


def softmax_sums(logits, block, turned_w):
    by_row = logits.T
    top = jnp.max(by_row, axis=1, keepdims=True)
    weights = jnp.exp(by_row - top)
    turned_w[...] = weights
    return top, dot(weights, block, HIGH)


def side(pair_ref, i, parity):
    _, far, _, half, width = pair_ref.shape
    return pair_ref[i, :, parity].reshape(far * half, width)


def pair_sums(turned_w, pair_ref, parity, g):
    width = pair_ref.shape[4]
    rows = slice(2 * SLOTS * g, 2 * SLOTS * (g + 1))
    right = jnp.concatenate(
        [side(pair_ref, 2 * g, parity), side(pair_ref, 2 * g + 1, parity)], axis=1
    )
    both = dot(turned_w[rows, :].astype(BF16), right)
    upper = iota((2 * SLOTS, width), 0) < SLOTS
    return rows, jnp.where(upper, both[:, :width], both[:, width:])


def near_kernel(
    heads,
    n_query,
    pair_ref,
    wb_hbm,
    mine_ref,
    qb_ref,
    qaux_ref,
    part_ref,
    bias_ref,
    weights,
    turned_w,
    wb_ref,
    sem,
):
    queries, far, _, half, width = pair_ref.shape
    keys = far * half
    place = lax.axis_index("blk") % 2
    small = pltpu.make_async_copy(wb_hbm, wb_ref, sem)
    small.start()
    block = mine_ref[...].reshape(keys, mine_ref.shape[2])
    partial, penalty = scores(n_query, block, qb_ref, qaux_ref)
    lane = iota((width, HALF), 1)
    row = iota((HALF, width), 0)
    small.wait()
    wb = wb_ref[...].astype(F32)
    each = jnp.zeros((HALF, width), F32)
    for h in range(heads):
        each = jnp.where(row % SLOTS == h, wb[h : h + 1, :], each)
    each = each.T
    for i in range(queries):
        weights[i * width : (i + 1) * width, :] = jnp.where(
            lane // SLOTS == i, each, 0.0
        ).astype(BF16)

    def bias_of(parity):
        left = jnp.concatenate([side(pair_ref, i, parity) for i in range(queries)], axis=1)
        return dot(left, weights[...])

    logits = (partial + LOGIT_WEIGHT * bias_of(place)) - penalty
    top, sums = softmax_sums(logits, block, turned_w)
    part_ref[:, HALF:] = jnp.where(iota(sums.shape, 1) == HALF + TOP, top, sums)
    for g in range(queries // 2):
        rows, found = pair_sums(turned_w, pair_ref, place, g)
        part_ref[rows, 0:width] = found
    bias_ref[...] = bias_of(1 - place)


def across_kernel(
    n_query, part_in, across_ref, bias_ref, qb_ref, qaux_ref, pair_ref, part_ref, turned_w
):
    far, half, lanes = across_ref.shape
    width = pair_ref.shape[4]
    place = lax.axis_index("blk") % 2
    block = across_ref[...].reshape(far * half, lanes)
    partial, penalty = scores(n_query, block, qb_ref, qaux_ref)
    logits = (partial + LOGIT_WEIGHT * bias_ref[...]) - penalty
    top, sums = softmax_sums(logits, block, turned_w)
    before = part_in[:, 2 * HALF + TOP : 2 * HALF + TOP + 1]
    best = jnp.maximum(before, top)
    old, new = jnp.exp(before - best), jnp.exp(top - best)
    merged = part_in[:, HALF:] * old + sums * new
    part_ref[:, HALF:] = jnp.where(iota(sums.shape, 1) == HALF + TOP, best, merged)
    for g in range(pair_ref.shape[0] // 2):
        rows, found = pair_sums(turned_w, pair_ref, 1 - place, g)
        part_ref[rows, 0:width] = part_in[rows, 0:width] * old[rows, :] + found * new[rows, :]


def merge_kernel(
    heads,
    size,
    n_value,
    mine_ref,
    theirs_ref,
    frows_ref,
    w_out_ref,
    out_ref,
    small,
    large,
):
    copies, rows, _ = out_ref.shape
    tops = [ref[:, 2 * HALF + TOP : 2 * HALF + TOP + 1] for ref in (mine_ref, theirs_ref)]
    sums = [ref[:, 2 * HALF + ONE : 2 * HALF + ONE + 1] for ref in (mine_ref, theirs_ref)]
    best = jnp.maximum(tops[0], tops[1])
    factors = [jnp.exp(top - best) for top in tops]
    total = factors[0] * sums[0] + factors[1] * sums[1]
    merged = (mine_ref[...] * factors[0] + theirs_ref[...] * factors[1]) / total
    slot = iota((HALF, 1), 0) % SLOTS

    def of_own_head(first, step, count):
        picked = jnp.zeros((HALF, count), F32)
        for h in range(heads):
            at = first + step * h
            picked = jnp.where(slot == h, merged[:, at : at + count], picked)
        return picked

    attended = of_own_head(HALF + size, 2 * size, size)
    moved = [
        of_own_head(2 * HALF + KEYED + heads * n_value * a, n_value, n_value)
        - frows_ref[:, 9 + a : 10 + a]
        for a in range(3)
    ]
    pointed = []
    for b in range(3):
        total_b = frows_ref[:, b : b + 1] * moved[0]
        for a in (1, 2):
            total_b += frows_ref[:, 3 * a + b : 3 * a + b + 1] * moved[a]
        pointed.append(total_b)
    norms = jnp.sqrt(
        pointed[0] * pointed[0] + pointed[1] * pointed[1] + pointed[2] * pointed[2] + 1.0
    )
    small[...] = jnp.zeros_like(small)
    small[:, 0:size] = attended
    for b in range(3):
        small[:, size + n_value * b : size + n_value * (b + 1)] = pointed[b]
    edge = size + 3 * n_value
    small[:, edge : edge + n_value] = norms
    source = iota((HALF, HALF), 0)
    target = iota((HALF, HALF), 1)
    inside = (source >= size) & (source < edge)
    goes = jnp.where(
        inside, size + 3 * ((source - size) % n_value) + (source - size) // n_value, source
    )
    order = (goes == target).astype(F32).astype(BF16)
    small[...] = dot(small[...].astype(BF16), order)
    large[...] = merged[:, :HALF]
    cut = edge + n_value
    update = jnp.zeros((rows, w_out_ref.shape[2]), F32)
    for h in range(heads):
        low = small[pl.ds(h, rows, stride=SLOTS), :].astype(BF16)
        update += dot(low[:, :cut], w_out_ref[h, 0:cut, :])
        wide = large[pl.ds(h, rows, stride=SLOTS), :].astype(BF16)
        update += dot(wide, w_out_ref[h, cut:, :])
    for k in range(copies):
        out_ref[k] = update


def finish_kernel(updates_ref, single_ref, gain_ref, wb_ref, frames_ref, out_ref, send_ref):
    copies, rows, channels = updates_ref.shape
    mixed = single_ref[...].astype(F32)
    update = updates_ref[0]
    for k in range(1, copies):
        update += updates_ref[k]
    mixed = mixed + update
    centre = jnp.mean(mixed, axis=1, keepdims=True)
    away = mixed - centre
    spread = jnp.mean(away * away, axis=1, keepdims=True)
    gain = gain_ref[...].reshape(1, channels)
    single_out = (away * lax.rsqrt(spread + 1e-05) * gain).astype(BF16)
    out_ref[...] = single_out
    motion = dot_nt(wb_ref[...], single_out)
    m = [motion[k : k + 1, :] for k in range(6)]
    qa = 1.0 / jnp.sqrt(1.0 + m[0] * m[0] + m[1] * m[1] + m[2] * m[2])
    qb, qc, qd = m[0] * qa, m[1] * qa, m[2] * qa
    spin = [
        [qa * qa + qb * qb - qc * qc - qd * qd, 2.0 * (qb * qc - qa * qd), 2.0 * (qb * qd + qa * qc)],
        [2.0 * (qb * qc + qa * qd), qa * qa - qb * qb + qc * qc - qd * qd, 2.0 * (qc * qd - qa * qb)],
        [2.0 * (qb * qd - qa * qc), 2.0 * (qc * qd + qa * qb), qa * qa - qb * qb - qc * qc + qd * qd],
    ]
    r = [[frames_ref[3 * a + b : 3 * a + b + 1, :] for b in range(3)] for a in range(3)]
    lines = []
    for a in range(3):
        for c in range(3):
            lines.append(r[a][0] * spin[0][c] + r[a][1] * spin[1][c] + r[a][2] * spin[2][c])
    for a in range(3):
        lines.append(
            frames_ref[9 + a : 10 + a, :] + (r[a][0] * m[3] + r[a][1] * m[4] + r[a][2] * m[5])
        )
    groups = HALF // rows
    repeat = (iota((rows, HALF), 1) % rows == iota((rows, HALF), 0)).astype(F32)
    wide = dot(jnp.concatenate(lines + lines[:4], axis=0), repeat, HIGH)
    group = iota((1, HALF), 1) // rows
    pieces = []
    for v in range(len(lines) // groups):
        piece = wide[groups * v : groups * v + 1, :]
        for s in range(1, groups):
            at = groups * v + s
            piece = jnp.where(group == s, wide[at : at + 1, :], piece)
        pieces.append(piece)
    line = jnp.concatenate(pieces, axis=1)
    send_ref[...] = jnp.broadcast_to(line, (send_ref.shape[0], line.shape[1])).reshape(
        send_ref.shape
    )


def spread_kernel(first, blocks_ref, out_ref):
    blocks, _, wide = blocks_ref.shape
    lines = out_ref.shape[0]
    rows = wide // lines
    groups = HALF // rows
    x = blocks_ref[...].reshape(blocks, wide)
    s = iota((blocks, HALF), 0) % groups
    g = iota((blocks, HALF), 1) // rows
    for v in range(wide // HALF):
        tile = x[:, HALF * v : HALF * (v + 1)]
        z = tile
        for d in range(1, groups):
            right = pltpu.roll(tile, rows * d, 1)
            up = pltpu.roll(right, blocks - d, 0)
            down = pltpu.roll(right, groups - d, 0)
            z = jnp.where(g - s == d, up, z)
            z = jnp.where(g - s == d - groups, down, z)
        for q in range(blocks // groups):
            at = (HALF * q + rows * first) % (rows * blocks)
            out_ref[groups * v : groups * (v + 1), at : at + HALF] = z[
                groups * q : groups * (q + 1), :
            ]


def in_hbm(x):
    return pltpu.with_memory_space_constraint(x, pltpu.HBM)


def call(kernel, outs, scratch=(), specs=None, n=0, room=4, cost=None, name=None):
    return pl.pallas_call(
        kernel,
        out_shape=outs,
        in_specs=specs or [VMEM] * n,
        out_specs=jax.tree.map(lambda _: VMEM, outs),
        scratch_shapes=list(scratch),
        cost_estimate=cost,
        compiler_params=pltpu.CompilerParams(vmem_limit_bytes=room * 1024 * 1024),
        name=name,
    )


def body(
    single,
    pair,
    frames,
    chain,
    mask,
    w_query,
    w_key_value,
    w_query_points,
    w_kv_points,
    w_pair_bias,
    head_weights,
    chain_bias,
    w_out,
    out_gain,
    w_backbone,
):
    rows, channels = single.shape
    blocks, half = pair.shape[1], pair.shape[2]
    width = pair.shape[3]
    heads = w_pair_bias.shape[1]
    size = w_query.shape[1] // heads
    n_query = w_query_points.shape[1] // (3 * heads)
    n_points = w_kv_points.shape[1] // (3 * heads)
    n_value = n_points - n_query
    keys = blocks * half
    shape = jax.ShapeDtypeStruct

    inputs = (single, frames, chain, mask, w_key_value.T, w_kv_points.T)
    payload = call(
        functools.partial(keys_kernel, heads, size, n_query, n_points),
        shape((half, 2 * HALF), F32),
        (
            pltpu.VMEM((3 * heads * n_points, rows), F32),
            pltpu.VMEM((HALF, rows), F32),
            pltpu.VMEM((rows, 2 * HALF), F32),
            *(pltpu.VMEM(x.shape, x.dtype) for x in inputs),
            pltpu.SemaphoreType.DMA((len(inputs),)),
        ),
        specs=[HBM] * len(inputs),
        cost=pl.CostEstimate(flops=10**10, bytes_accessed=4 * pair.size, transcendentals=0),
        name="keys",
    )(*(in_hbm(x) for x in inputs))
    ways = [list(range(k, blocks, 2)) for k in range(2)]
    gathered = lax.all_gather(payload, "blk", axis=0, axis_index_groups=ways, tiled=False)
    swap = [(k, k + 1 - 2 * (k % 2)) for k in range(blocks)]
    across = lax.ppermute(gathered, "blk", swap)
    qb, qaux, frows = call(
        functools.partial(queries_kernel, heads, size, n_query),
        (shape((HALF, HALF), F32), shape((16, HALF), F32), shape((HALF, HALF), F32)),
        (
            pltpu.VMEM((3 * heads * n_query, rows), F32),
            pltpu.VMEM((HALF, rows), F32),
            pltpu.VMEM((104, rows), F32),
        ),
        specs=[VMEM] * 6 + [SMEM] * 2,
        cost=pl.CostEstimate(flops=10**8, bytes_accessed=10**5, transcendentals=0),
        name="queries",
    )(single, frames, chain, mask, w_query.T, w_query_points.T, head_weights, chain_bias)
    halves = pair.reshape(rows, blocks // 2, 2, half, width)
    part, bias = call(
        functools.partial(near_kernel, heads, n_query),
        (shape((HALF, 3 * HALF), F32), shape((keys // 2, HALF), F32)),
        (
            pltpu.VMEM((rows * width, HALF), BF16),
            pltpu.VMEM((HALF, keys // 2), F32),
            pltpu.VMEM((heads, width), w_pair_bias.dtype),
            pltpu.SemaphoreType.DMA,
        ),
        specs=[VMEM, HBM, VMEM, VMEM, VMEM],
        room=16,
        cost=pl.CostEstimate(flops=10**9, bytes_accessed=2 * pair.size, transcendentals=0),
        name="near",
    )(halves, in_hbm(w_pair_bias.T), gathered, qb, qaux)
    part = call(
        functools.partial(across_kernel, n_query),
        shape((HALF, 3 * HALF), F32),
        (pltpu.VMEM((HALF, keys // 2), F32),),
        n=6,
        room=16,
        name="across",
    )(part, across, bias, qb, qaux, halves)
    other = lax.ppermute(part, "pair", [(0, 1), (1, 0)])
    updates = call(
        functools.partial(merge_kernel, heads, size, n_value),
        shape((lax.axis_size("head"), rows, channels), F32),
        (pltpu.VMEM((HALF, HALF), F32), pltpu.VMEM((HALF, HALF), F32)),
        n=4,
        name="merge",
    )(part, other, frows, w_out)
    updates = lax.all_to_all(updates, "head", split_axis=0, concat_axis=0, tiled=True)
    single_out, send = call(
        finish_kernel,
        (shape((rows, channels), BF16), shape((blocks, 1, 12 * rows), F32)),
        n=5,
        name="finish",
    )(updates, single, out_gain, w_backbone.T, frames)
    middle_first = [(k + blocks // 2) % blocks for k in range(blocks)]
    received = lax.all_to_all(
        send, "blk", split_axis=0, concat_axis=0, axis_index_groups=[middle_first], tiled=True
    )
    frames_out = call(
        functools.partial(spread_kernel, middle_first[0]),
        shape((12, blocks * rows), F32),
        n=1,
        name="spread",
    )(received)
    return (single_out, frames_out)


def solution(mesh):
    split = ("groups", "blk")
    placed = (
        P(split, None),
        P(split, None, "pair", None),
        P(None, split),
        P(split),
        P(split),
        P(None, "head"),
        P(None, "head"),
        P(None, "head"),
        P(None, "head"),
        P(None, "head"),
        P("head"),
        P("head"),
        P("head", None, None),
        P(),
        P(),
    )
    return jax.shard_map(
        body,
        mesh=mesh,
        in_specs=placed,
        out_specs=(P(split, None), P(None, "groups")),
        check_vma=False,
    )
```

```python
import functools
import math

import jax
import jax.numpy as jnp
from jax import lax
from jax.experimental import pallas as pl
from jax.experimental.pallas import tpu as pltpu
from jax.sharding import PartitionSpec as P

HIGH = lax.Precision.HIGHEST
LOGIT_WEIGHT = math.sqrt(1.0 / 3.0)
MASK_PENALTY = 100000.0
F32 = jnp.float32
BF16 = jnp.bfloat16

SLOTS = 4
HALF = 128
KEYED = 40
CHAIN, PRESENT, ONE, TOP = 36, 37, 38, 39
VMEM = pl.BlockSpec(memory_space=pltpu.VMEM)
SMEM = pl.BlockSpec(memory_space=pltpu.SMEM)
HBM = pl.BlockSpec(memory_space=pltpu.HBM)


def iota(shape, dim):
    return lax.broadcasted_iota(jnp.int32, shape, dim)


def dot(a, b, precision=None):
    return jnp.dot(a, b, preferred_element_type=F32, precision=precision)


def dot_nt(a, b):
    return lax.dot_general(a, b, (((1,), (1,)), ((), ())), preferred_element_type=F32)


def rotated(frames_ref, parts):
    moved = []
    for a in range(3):
        total = frames_ref[3 * a : 3 * a + 1, :] * parts[0]
        for b in (1, 2):
            total += frames_ref[3 * a + b : 3 * a + b + 1, :] * parts[b]
        moved.append(total + frames_ref[9 + a : 10 + a, :])
    return moved


def keys_kernel(heads, size, n_query, n_points, *refs):
    sources, refs = refs[:6], refs[6:]
    payload_ref, turned, points, full, spare = refs[:5]
    local_refs, sem = refs[5:11], refs[11]
    copies = [
        pltpu.make_async_copy(source, target, sem.at[k])
        for k, (source, target) in enumerate(zip(sources, local_refs))
    ]
    for copy in copies:
        copy.start()
    single_ref, frames_ref, chain_ref, mask_ref, wkv_ref, wkp_ref = local_refs
    spare[...] = jnp.zeros_like(spare)
    points[...] = jnp.zeros_like(points)
    for copy in copies:
        copy.wait()
    rows = single_ref.shape[0]
    half = payload_ref.shape[0]
    n_value = n_points - n_query
    x = single_ref[...]
    turned[...] = dot_nt(wkp_ref[...], x)
    edge = 2 * heads * size
    values = frames_ref[...]
    spare[edge : edge + 12, :] = values
    spare[edge + 12 : edge + 24, :] = jnp.concatenate([values[:, half:], values[:, :half]], axis=1)
    full[:, :HALF] = spare[...].T
    full[:, 0:edge] = dot_nt(x, wkv_ref[...])
    count = heads * n_points
    local = [turned[pl.ds(b, count, stride=3), :] for b in range(3)]
    for a, value in enumerate(rotated(frames_ref, local)):
        for h in range(heads):
            at = heads * n_query * a + n_query * h
            points[at : at + n_query, :] = value[n_points * h : n_points * h + n_query, :]
            at = KEYED + heads * n_value * a + n_value * h
            points[at : at + n_value, :] = value[n_points * h + n_query : n_points * (h + 1), :]
    points[CHAIN : CHAIN + 1, :] = chain_ref[...].astype(F32).reshape(1, rows)
    points[PRESENT : PRESENT + 1, :] = mask_ref[...].astype(F32).reshape(1, rows)
    points[ONE : ONE + 1, :] = jnp.ones((1, rows), F32)
    full[:, HALF:] = points[...].T
    start = pl.multiple_of(lax.axis_index("pair") * half, half)
    payload_ref[...] = full[pl.ds(start, half), :]


def queries_kernel(
    heads,
    size,
    n_query,
    single_ref,
    frames_ref,
    chain_ref,
    mask_ref,
    wq_ref,
    wqp_ref,
    hw_ref,
    cb_ref,
    qb_ref,
    qaux_ref,
    frows_ref,
    turned,
    points,
    spread,
):
    rows = single_ref.shape[0]
    x = single_ref[...]
    turned[...] = dot_nt(wqp_ref[...], x)
    count = heads * n_query
    local = [turned[pl.ds(b, count, stride=3), :] for b in range(3)]
    spread[...] = jnp.zeros_like(spread)
    spread[0 : heads * size, :] = dot_nt(wq_ref[...], x)
    for a, value in enumerate(rotated(frames_ref, local)):
        spread[48 + 16 * a : 48 + 16 * a + count, :] = value
    spread[96:97, :] = chain_ref[...].astype(F32).reshape(1, rows)
    spread[97:98, :] = mask_ref[...].astype(F32).reshape(1, rows)
    to_slots = (iota((rows, HALF), 1) // SLOTS == iota((rows, HALF), 0)).astype(F32)
    wide = dot(spread[...], to_slots, HIGH)
    slot = iota((1, HALF), 1) % SLOTS
    qb_ref[...] = jnp.zeros_like(qb_ref)
    scale = LOGIT_WEIGHT / math.sqrt(size)
    for h in range(heads):
        block = wide[h * size : (h + 1) * size, :] * scale
        qb_ref[2 * size * h : 2 * size * h + size, :] = jnp.where(slot == h, block, 0.0)
    qaux_ref[...] = jnp.zeros_like(qaux_ref)
    for a in range(3):
        for p in range(n_query):
            line = jnp.zeros((1, HALF), F32)
            for h in range(heads):
                at = 48 + 16 * a + h * n_query + p
                line = jnp.where(slot == h, wide[at : at + 1, :], line)
            qaux_ref[n_query * a + p : n_query * a + p + 1, :] = line
    raw = jnp.zeros((1, HALF), F32)
    bonus = jnp.zeros((1, HALF), F32)
    for h in range(heads):
        raw = jnp.where(slot == h, hw_ref[h], raw)
        bonus = jnp.where(slot == h, cb_ref[h], bonus)
    soft = jnp.maximum(raw, 0.0) + jnp.log1p(jnp.exp(-jnp.abs(raw)))
    used = 3 * n_query
    qaux_ref[used : used + 1, :] = soft * (math.sqrt(2.0 / (9.0 * n_query)) / 2.0)
    qaux_ref[used + 1 : used + 2, :] = bonus
    qaux_ref[used + 2 : used + 3, :] = wide[96:97, :]
    qaux_ref[used + 3 : used + 4, :] = wide[97:98, :]
    points[...] = jnp.zeros_like(points)
    points[0:12, :] = frames_ref[...]
    to_rows = (iota((HALF, rows), 0) // SLOTS == iota((HALF, rows), 1)).astype(F32)
    frows_ref[...] = dot(to_rows, points[...].T, HIGH)


def scores(n_query, block, qb_ref, qaux_ref):
    keep = iota((block.shape[0], HALF), 1) < KEYED
    high = jnp.where(keep, block[:, HALF:], 0.0)
    first = high.astype(BF16).astype(F32)
    rest = high - first
    second = rest.astype(BF16).astype(F32)
    third = (rest - second).astype(BF16).astype(F32)
    split = first + pltpu.roll(second, KEYED, 1) + pltpu.roll(third, 2 * KEYED, 1)
    split = split.astype(BF16)
    row = iota((HALF, HALF), 0)
    lane = iota((HALF, HALF), 1)
    slot = lane % SLOTS
    heads = CHAIN // (3 * n_query)
    wanted = [
        jnp.where(slot < heads, n_query * (heads * a + slot) + p, -1)
        for a in range(3)
        for p in range(n_query)
    ]
    wanted += [jnp.full((HALF, HALF), CHAIN), jnp.full((HALF, HALF), PRESENT)]
    found = []
    for k in range(0, len(wanted), 2):
        picks = [
            ((row % KEYED == w) & (row < 3 * KEYED)).astype(F32).astype(BF16)
            for w in wanted[k : k + 2]
        ]
        both = dot(split, jnp.concatenate(picks, axis=1))
        found += [both[:, :HALF], both[:, HALF:]]
    used = 3 * n_query
    distance = jnp.zeros((block.shape[0], HALF), F32)
    for k in range(used):
        gap = qaux_ref[k : k + 1, :] - found[k]
        distance += gap * gap
    scale = qaux_ref[used : used + 1, :]
    bonus = qaux_ref[used + 1 : used + 2, :]
    differ = found[used] != qaux_ref[used + 2 : used + 3, :]
    there = found[used + 1] * qaux_ref[used + 3 : used + 4, :]
    partial = dot(block[:, :HALF], qb_ref[...], HIGH) + LOGIT_WEIGHT * (
        jnp.where(differ, bonus, 0.0) - scale * distance
    )
    return partial, MASK_PENALTY * (1.0 - there)


def softmax_sums(logits, block, turned_w):
    by_row = logits.T
    top = jnp.max(by_row, axis=1, keepdims=True)
    weights = jnp.exp(by_row - top)
    turned_w[...] = weights
    return top, dot(weights, block, HIGH)


def side(pair_ref, i, parity):
    _, far, _, half, width = pair_ref.shape
    return pair_ref[i, :, parity].reshape(far * half, width)


def pair_sums(turned_w, pair_ref, parity, g):
    width = pair_ref.shape[4]
    rows = slice(2 * SLOTS * g, 2 * SLOTS * (g + 1))
    right = jnp.concatenate(
        [side(pair_ref, 2 * g, parity), side(pair_ref, 2 * g + 1, parity)], axis=1
    )
    both = dot(turned_w[rows, :].astype(BF16), right)
    upper = iota((2 * SLOTS, width), 0) < SLOTS
    return rows, jnp.where(upper, both[:, :width], both[:, width:])


def near_kernel(
    heads,
    n_query,
    pair_ref,
    wb_hbm,
    mine_ref,
    qb_ref,
    qaux_ref,
    part_ref,
    bias_ref,
    weights,
    turned_w,
    wb_ref,
    sem,
):
    queries, far, _, half, width = pair_ref.shape
    keys = far * half
    place = lax.axis_index("blk") % 2
    small = pltpu.make_async_copy(wb_hbm, wb_ref, sem)
    small.start()
    block = mine_ref[...].reshape(keys, mine_ref.shape[2])
    partial, penalty = scores(n_query, block, qb_ref, qaux_ref)
    lane = iota((width, HALF), 1)
    row = iota((HALF, width), 0)
    small.wait()
    wb = wb_ref[...].astype(F32)
    each = jnp.zeros((HALF, width), F32)
    for h in range(heads):
        each = jnp.where(row % SLOTS == h, wb[h : h + 1, :], each)
    each = each.T
    for i in range(queries):
        weights[i * width : (i + 1) * width, :] = jnp.where(
            lane // SLOTS == i, each, 0.0
        ).astype(BF16)

    def bias_of(parity):
        left = jnp.concatenate([side(pair_ref, i, parity) for i in range(queries)], axis=1)
        return dot(left, weights[...])

    logits = (partial + LOGIT_WEIGHT * bias_of(place)) - penalty
    top, sums = softmax_sums(logits, block, turned_w)
    part_ref[:, HALF:] = jnp.where(iota(sums.shape, 1) == HALF + TOP, top, sums)
    for g in range(queries // 2):
        rows, found = pair_sums(turned_w, pair_ref, place, g)
        part_ref[rows, 0:width] = found
    bias_ref[...] = bias_of(1 - place)


def across_kernel(
    n_query, part_in, across_ref, bias_ref, qb_ref, qaux_ref, pair_ref, part_ref, turned_w
):
    far, half, lanes = across_ref.shape
    width = pair_ref.shape[4]
    place = lax.axis_index("blk") % 2
    block = across_ref[...].reshape(far * half, lanes)
    partial, penalty = scores(n_query, block, qb_ref, qaux_ref)
    logits = (partial + LOGIT_WEIGHT * bias_ref[...]) - penalty
    top, sums = softmax_sums(logits, block, turned_w)
    before = part_in[:, 2 * HALF + TOP : 2 * HALF + TOP + 1]
    best = jnp.maximum(before, top)
    old, new = jnp.exp(before - best), jnp.exp(top - best)
    merged = part_in[:, HALF:] * old + sums * new
    part_ref[:, HALF:] = jnp.where(iota(sums.shape, 1) == HALF + TOP, best, merged)
    for g in range(pair_ref.shape[0] // 2):
        rows, found = pair_sums(turned_w, pair_ref, 1 - place, g)
        part_ref[rows, 0:width] = part_in[rows, 0:width] * old[rows, :] + found * new[rows, :]


def merge_kernel(
    heads,
    size,
    n_value,
    mine_ref,
    theirs_ref,
    frows_ref,
    w_out_ref,
    _,
    out_ref,
    small,
    large,
):
    copies, rows, _ = out_ref.shape
    tops = [ref[:, 2 * HALF + TOP : 2 * HALF + TOP + 1] for ref in (mine_ref, theirs_ref)]
    sums = [ref[:, 2 * HALF + ONE : 2 * HALF + ONE + 1] for ref in (mine_ref, theirs_ref)]
    best = jnp.maximum(tops[0], tops[1])
    factors = [jnp.exp(top - best) for top in tops]
    total = factors[0] * sums[0] + factors[1] * sums[1]
    merged = (mine_ref[...] * factors[0] + theirs_ref[...] * factors[1]) / total
    slot = iota((HALF, 1), 0) % SLOTS

    def of_own_head(first, step, count):
        picked = jnp.zeros((HALF, count), F32)
        for h in range(heads):
            at = first + step * h
            picked = jnp.where(slot == h, merged[:, at : at + count], picked)
        return picked

    attended = of_own_head(HALF + size, 2 * size, size)
    moved = [
        of_own_head(2 * HALF + KEYED + heads * n_value * a, n_value, n_value)
        - frows_ref[:, 9 + a : 10 + a]
        for a in range(3)
    ]
    pointed = []
    for b in range(3):
        total_b = frows_ref[:, b : b + 1] * moved[0]
        for a in (1, 2):
            total_b += frows_ref[:, 3 * a + b : 3 * a + b + 1] * moved[a]
        pointed.append(total_b)
    norms = jnp.sqrt(
        pointed[0] * pointed[0] + pointed[1] * pointed[1] + pointed[2] * pointed[2] + 1.0
    )
    small[...] = jnp.zeros_like(small)
    small[:, 0:size] = attended
    for b in range(3):
        small[:, size + n_value * b : size + n_value * (b + 1)] = pointed[b]
    edge = size + 3 * n_value
    small[:, edge : edge + n_value] = norms
    source = iota((HALF, HALF), 0)
    target = iota((HALF, HALF), 1)
    inside = (source >= size) & (source < edge)
    goes = jnp.where(
        inside, size + 3 * ((source - size) % n_value) + (source - size) // n_value, source
    )
    order = (goes == target).astype(F32).astype(BF16)
    small[...] = dot(small[...].astype(BF16), order)
    large[...] = merged[:, :HALF]
    cut = edge + n_value
    update = jnp.zeros((rows, w_out_ref.shape[2]), F32)
    for h in range(heads):
        low = small[pl.ds(h, rows, stride=SLOTS), :].astype(BF16)
        update += dot(low[:, :cut], w_out_ref[h, 0:cut, :])
        wide = large[pl.ds(h, rows, stride=SLOTS), :].astype(BF16)
        update += dot(wide, w_out_ref[h, cut:, :])
    for k in range(copies):
        out_ref[k] = update


def finish_kernel(updates_ref, single_ref, gain_ref, wb_ref, out_ref, send_ref):
    copies, rows, channels = updates_ref.shape
    mixed = single_ref[...].astype(F32)
    update = updates_ref[0]
    for k in range(1, copies):
        update += updates_ref[k]
    mixed = mixed + update
    centre = jnp.mean(mixed, axis=1, keepdims=True)
    away = mixed - centre
    spread = jnp.mean(away * away, axis=1, keepdims=True)
    gain = gain_ref[...].reshape(1, channels)
    single_out = (away * lax.rsqrt(spread + 1e-05) * gain).astype(BF16)
    out_ref[...] = single_out
    motion = dot_nt(wb_ref[...], single_out)
    groups = HALF // rows
    repeat = (iota((rows, HALF), 1) % rows == iota((rows, HALF), 0)).astype(F32)
    wide = dot(jnp.concatenate([motion, motion[:2]], axis=0), repeat, HIGH)
    group = iota((1, HALF), 1) // rows
    pieces = []
    for v in range(wide.shape[0] // groups):
        piece = wide[groups * v : groups * v + 1, :]
        for s in range(1, groups):
            at = groups * v + s
            piece = jnp.where(group == s, wide[at : at + 1, :], piece)
        pieces.append(piece)
    line = jnp.concatenate(pieces, axis=1)
    send_ref[...] = jnp.broadcast_to(line, (send_ref.shape[0], line.shape[1])).reshape(
        send_ref.shape
    )


def frames_kernel(edge, mine_ref, across_ref, out_ref, order):
    far, half, _ = mine_ref.shape
    place = lax.axis_index("blk") % 2
    which = lax.axis_index("pair")
    for ref, parity in ((mine_ref, place), (across_ref, 1 - place)):
        x = ref[:, :, :HALF].reshape(far * half, HALF)
        own = pltpu.roll(x, HALF - edge, 1)
        other = pltpu.roll(x, HALF - edge - 12, 1)
        for k in range(far):
            base = (2 * k + parity) * 2 * half
            rows = slice(k * half, (k + 1) * half)
            order[pl.ds(pl.multiple_of(base + which * half, half), half), :] = own[rows, :]
            order[pl.ds(pl.multiple_of(base + (1 - which) * half, half), half), :] = other[rows, :]
    for q in range(4 * far * half // HALF):
        at = slice(HALF * q, HALF * (q + 1))
        out_ref[:, at] = order[at, :].T[0:12, :]


def spread_kernel(first, blocks_ref, frames_ref, single_ref, out_ref, single_out_ref, motion):
    single_out_ref[...] = single_ref[...]
    blocks, _, wide = blocks_ref.shape
    rows = frames_ref.shape[1] // blocks
    groups = HALF // rows
    x = blocks_ref[...].reshape(blocks, wide)
    s = iota((blocks, HALF), 0) % groups
    g = iota((blocks, HALF), 1) // rows
    for v in range(wide // HALF):
        tile = x[:, HALF * v : HALF * (v + 1)]
        z = tile
        for d in range(1, groups):
            right = pltpu.roll(tile, rows * d, 1)
            up = pltpu.roll(right, blocks - d, 0)
            down = pltpu.roll(right, groups - d, 0)
            z = jnp.where(g - s == d, up, z)
            z = jnp.where(g - s == d - groups, down, z)
        for q in range(blocks // groups):
            at = (HALF * q + rows * first) % (rows * blocks)
            motion[groups * v : groups * (v + 1), at : at + HALF] = z[
                groups * q : groups * (q + 1), :
            ]
    m = [motion[k : k + 1, :] for k in range(6)]
    qa = 1.0 / jnp.sqrt(1.0 + m[0] * m[0] + m[1] * m[1] + m[2] * m[2])
    qb, qc, qd = m[0] * qa, m[1] * qa, m[2] * qa
    spin = [
        [qa * qa + qb * qb - qc * qc - qd * qd, 2.0 * (qb * qc - qa * qd), 2.0 * (qb * qd + qa * qc)],
        [2.0 * (qb * qc + qa * qd), qa * qa - qb * qb + qc * qc - qd * qd, 2.0 * (qc * qd - qa * qb)],
        [2.0 * (qb * qd - qa * qc), 2.0 * (qc * qd + qa * qb), qa * qa - qb * qb - qc * qc + qd * qd],
    ]
    for a in range(3):
        r = [frames_ref[3 * a + b : 3 * a + b + 1, :] for b in range(3)]
        for c in range(3):
            line = r[0] * spin[0][c] + r[1] * spin[1][c] + r[2] * spin[2][c]
            out_ref[3 * a + c : 3 * a + c + 1, :] = line
        moved = r[0] * m[3] + r[1] * m[4] + r[2] * m[5]
        out_ref[9 + a : 10 + a, :] = frames_ref[9 + a : 10 + a, :] + moved


def in_hbm(x):
    return pltpu.with_memory_space_constraint(x, pltpu.HBM)


def call(kernel, outs, scratch=(), specs=None, n=0, room=4, cost=None, name=None):
    return pl.pallas_call(
        kernel,
        out_shape=outs,
        in_specs=specs or [VMEM] * n,
        out_specs=jax.tree.map(lambda _: VMEM, outs),
        scratch_shapes=list(scratch),
        cost_estimate=cost,
        compiler_params=pltpu.CompilerParams(vmem_limit_bytes=room * 1024 * 1024),
        name=name,
    )


def body(
    single,
    pair,
    frames,
    chain,
    mask,
    w_query,
    w_key_value,
    w_query_points,
    w_kv_points,
    w_pair_bias,
    head_weights,
    chain_bias,
    w_out,
    out_gain,
    w_backbone,
):
    rows, channels = single.shape
    blocks, half = pair.shape[1], pair.shape[2]
    width = pair.shape[3]
    heads = w_pair_bias.shape[1]
    size = w_query.shape[1] // heads
    n_query = w_query_points.shape[1] // (3 * heads)
    n_points = w_kv_points.shape[1] // (3 * heads)
    n_value = n_points - n_query
    keys = blocks * half
    shape = jax.ShapeDtypeStruct

    inputs = (single, frames, chain, mask, w_key_value.T, w_kv_points.T)
    payload = call(
        functools.partial(keys_kernel, heads, size, n_query, n_points),
        shape((half, 2 * HALF), F32),
        (
            pltpu.VMEM((3 * heads * n_points, rows), F32),
            pltpu.VMEM((HALF, rows), F32),
            pltpu.VMEM((rows, 2 * HALF), F32),
            pltpu.VMEM((HALF, rows), F32),
            *(pltpu.VMEM(x.shape, x.dtype) for x in inputs),
            pltpu.SemaphoreType.DMA((len(inputs),)),
        ),
        specs=[HBM] * len(inputs),
        cost=pl.CostEstimate(flops=10**10, bytes_accessed=4 * pair.size, transcendentals=0),
        name="keys",
    )(*(in_hbm(x) for x in inputs))
    ways = [list(range(k, blocks, 2)) for k in range(2)]
    gathered = lax.all_gather(payload, "blk", axis=0, axis_index_groups=ways, tiled=False)
    swap = [(k, k + 1 - 2 * (k % 2)) for k in range(blocks)]
    across = lax.ppermute(gathered, "blk", swap)
    qb, qaux, frows = call(
        functools.partial(queries_kernel, heads, size, n_query),
        (shape((HALF, HALF), F32), shape((16, HALF), F32), shape((HALF, HALF), F32)),
        (
            pltpu.VMEM((3 * heads * n_query, rows), F32),
            pltpu.VMEM((HALF, rows), F32),
            pltpu.VMEM((104, rows), F32),
        ),
        specs=[VMEM] * 6 + [SMEM] * 2,
        cost=pl.CostEstimate(flops=10**8, bytes_accessed=10**5, transcendentals=0),
        name="queries",
    )(single, frames, chain, mask, w_query.T, w_query_points.T, head_weights, chain_bias)
    halves = pair.reshape(rows, blocks // 2, 2, half, width)
    part, bias = call(
        functools.partial(near_kernel, heads, n_query),
        (shape((HALF, 3 * HALF), F32), shape((keys // 2, HALF), F32)),
        (
            pltpu.VMEM((rows * width, HALF), BF16),
            pltpu.VMEM((HALF, keys // 2), F32),
            pltpu.VMEM((heads, width), w_pair_bias.dtype),
            pltpu.SemaphoreType.DMA,
        ),
        specs=[VMEM, HBM, VMEM, VMEM, VMEM],
        room=16,
        cost=pl.CostEstimate(flops=10**9, bytes_accessed=2 * pair.size, transcendentals=0),
        name="near",
    )(halves, in_hbm(w_pair_bias.T), gathered, qb, qaux)
    part = call(
        functools.partial(across_kernel, n_query),
        shape((HALF, 3 * HALF), F32),
        (pltpu.VMEM((HALF, keys // 2), F32),),
        n=6,
        room=16,
        name="across",
    )(part, across, bias, qb, qaux, halves)
    other = lax.ppermute(part, "pair", [(0, 1), (1, 0)])
    all_frames = call(
        functools.partial(frames_kernel, 2 * heads * size),
        shape((12, blocks * rows), F32),
        (pltpu.VMEM((blocks * rows, HALF), F32),),
        n=2,
        cost=pl.CostEstimate(flops=10**8, bytes_accessed=10**6, transcendentals=0),
        name="frames",
    )(gathered, across)
    updates = call(
        functools.partial(merge_kernel, heads, size, n_value),
        shape((lax.axis_size("head"), rows, channels), F32),
        (pltpu.VMEM((HALF, HALF), F32), pltpu.VMEM((HALF, HALF), F32)),
        n=5,
        name="merge",
    )(part, other, frows, w_out, all_frames)
    sides = lax.axis_size("head")
    last_first = [(k + sides - 1) % sides for k in range(sides)]
    updates = lax.all_to_all(
        updates, "head", split_axis=0, concat_axis=0, axis_index_groups=[last_first], tiled=True
    )
    single_here, send = call(
        finish_kernel,
        (shape((rows, channels), BF16), shape((blocks, 1, 8 * rows), F32)),
        n=4,
        name="finish",
    )(updates, single, out_gain, w_backbone.T)
    middle_first = [(k + blocks // 2) % blocks for k in range(blocks)]
    received = lax.all_to_all(
        send, "blk", split_axis=0, concat_axis=0, axis_index_groups=[middle_first], tiled=True
    )
    frames_out, single_out = call(
        functools.partial(spread_kernel, middle_first[0]),
        (shape((12, blocks * rows), F32), shape((rows, channels), BF16)),
        (pltpu.VMEM((8, blocks * rows), F32),),
        n=3,
        name="spread",
    )(received, all_frames, single_here)
    return (single_out, frames_out)


def solution(mesh):
    split = ("groups", "blk")
    placed = (
        P(split, None),
        P(split, None, "pair", None),
        P(None, split),
        P(split),
        P(split),
        P(None, "head"),
        P(None, "head"),
        P(None, "head"),
        P(None, "head"),
        P(None, "head"),
        P("head"),
        P("head"),
        P("head", None, None),
        P(),
        P(),
    )
    return jax.shard_map(
        body,
        mesh=mesh,
        in_specs=placed,
        out_specs=(P(split, None), P(None, "groups")),
        check_vma=False,
    )
```

```python
import functools
import math

import jax
import jax.numpy as jnp
from jax import lax
from jax.experimental import pallas as pl
from jax.experimental.pallas import tpu as pltpu
from jax.sharding import PartitionSpec as P

HIGH = lax.Precision.HIGHEST
LOGIT_WEIGHT = math.sqrt(1.0 / 3.0)
MASK_PENALTY = 100000.0
F32 = jnp.float32
BF16 = jnp.bfloat16

SLOTS = 4
HALF = 128
KEYED = 40
CHAIN, PRESENT, ONE, TOP = 36, 37, 38, 39
VMEM = pl.BlockSpec(memory_space=pltpu.VMEM)
SMEM = pl.BlockSpec(memory_space=pltpu.SMEM)
HBM = pl.BlockSpec(memory_space=pltpu.HBM)


def iota(shape, dim):
    return lax.broadcasted_iota(jnp.int32, shape, dim)


def dot(a, b, precision=None):
    return jnp.dot(a, b, preferred_element_type=F32, precision=precision)


def dot_nt(a, b):
    return lax.dot_general(a, b, (((1,), (1,)), ((), ())), preferred_element_type=F32)


def rotated(frames_ref, parts):
    moved = []
    for a in range(3):
        total = frames_ref[3 * a : 3 * a + 1, :] * parts[0]
        for b in (1, 2):
            total += frames_ref[3 * a + b : 3 * a + b + 1, :] * parts[b]
        moved.append(total + frames_ref[9 + a : 10 + a, :])
    return moved


def keys_kernel(heads, size, n_query, n_points, *refs):
    sources, refs = refs[:6], refs[6:]
    payload_ref, turned, points, full, spare = refs[:5]
    local_refs, sem = refs[5:11], refs[11]
    copies = [
        pltpu.make_async_copy(source, target, sem.at[k])
        for k, (source, target) in enumerate(zip(sources, local_refs))
    ]
    for copy in copies:
        copy.start()
    single_ref, frames_ref, chain_ref, mask_ref, wkv_ref, wkp_ref = local_refs
    spare[...] = jnp.zeros_like(spare)
    points[...] = jnp.zeros_like(points)
    for copy in copies:
        copy.wait()
    rows = single_ref.shape[0]
    half = payload_ref.shape[0]
    n_value = n_points - n_query
    x = single_ref[...]
    turned[...] = dot_nt(wkp_ref[...], x)
    edge = 2 * heads * size
    values = frames_ref[...]
    spare[edge : edge + 12, :] = values
    spare[edge + 12 : edge + 24, :] = jnp.concatenate([values[:, half:], values[:, :half]], axis=1)
    full[:, :HALF] = spare[...].T
    full[:, 0:edge] = dot_nt(x, wkv_ref[...])
    count = heads * n_points
    local = [turned[pl.ds(b, count, stride=3), :] for b in range(3)]
    for a, value in enumerate(rotated(frames_ref, local)):
        for h in range(heads):
            at = heads * n_query * a + n_query * h
            points[at : at + n_query, :] = value[n_points * h : n_points * h + n_query, :]
            at = KEYED + heads * n_value * a + n_value * h
            points[at : at + n_value, :] = value[n_points * h + n_query : n_points * (h + 1), :]
    points[CHAIN : CHAIN + 1, :] = chain_ref[...].astype(F32).reshape(1, rows)
    points[PRESENT : PRESENT + 1, :] = mask_ref[...].astype(F32).reshape(1, rows)
    points[ONE : ONE + 1, :] = jnp.ones((1, rows), F32)
    full[:, HALF:] = points[...].T
    start = pl.multiple_of(lax.axis_index("pair") * half, half)
    payload_ref[...] = full[pl.ds(start, half), :]


def queries_kernel(
    heads,
    size,
    n_query,
    single_ref,
    frames_ref,
    chain_ref,
    mask_ref,
    wq_ref,
    wqp_ref,
    hw_ref,
    cb_ref,
    qb_ref,
    qaux_ref,
    frows_ref,
    turned,
    points,
    spread,
):
    rows = single_ref.shape[0]
    x = single_ref[...]
    turned[...] = dot_nt(wqp_ref[...], x)
    count = heads * n_query
    local = [turned[pl.ds(b, count, stride=3), :] for b in range(3)]
    spread[...] = jnp.zeros_like(spread)
    spread[0 : heads * size, :] = dot_nt(wq_ref[...], x)
    for a, value in enumerate(rotated(frames_ref, local)):
        spread[48 + 16 * a : 48 + 16 * a + count, :] = value
    spread[96:97, :] = chain_ref[...].astype(F32).reshape(1, rows)
    spread[97:98, :] = mask_ref[...].astype(F32).reshape(1, rows)
    to_slots = (iota((rows, HALF), 1) // SLOTS == iota((rows, HALF), 0)).astype(F32)
    wide = dot(spread[...], to_slots, HIGH)
    slot = iota((1, HALF), 1) % SLOTS
    qb_ref[...] = jnp.zeros_like(qb_ref)
    scale = LOGIT_WEIGHT / math.sqrt(size)
    for h in range(heads):
        block = wide[h * size : (h + 1) * size, :] * scale
        qb_ref[2 * size * h : 2 * size * h + size, :] = jnp.where(slot == h, block, 0.0)
    qaux_ref[...] = jnp.zeros_like(qaux_ref)
    for a in range(3):
        for p in range(n_query):
            line = jnp.zeros((1, HALF), F32)
            for h in range(heads):
                at = 48 + 16 * a + h * n_query + p
                line = jnp.where(slot == h, wide[at : at + 1, :], line)
            qaux_ref[n_query * a + p : n_query * a + p + 1, :] = line
    raw = jnp.zeros((1, HALF), F32)
    bonus = jnp.zeros((1, HALF), F32)
    for h in range(heads):
        raw = jnp.where(slot == h, hw_ref[h], raw)
        bonus = jnp.where(slot == h, cb_ref[h], bonus)
    soft = jnp.maximum(raw, 0.0) + jnp.log1p(jnp.exp(-jnp.abs(raw)))
    used = 3 * n_query
    qaux_ref[used : used + 1, :] = soft * (math.sqrt(2.0 / (9.0 * n_query)) / 2.0)
    qaux_ref[used + 1 : used + 2, :] = bonus
    qaux_ref[used + 2 : used + 3, :] = wide[96:97, :]
    qaux_ref[used + 3 : used + 4, :] = wide[97:98, :]
    points[...] = jnp.zeros_like(points)
    points[0:12, :] = frames_ref[...]
    to_rows = (iota((HALF, rows), 0) // SLOTS == iota((HALF, rows), 1)).astype(F32)
    frows_ref[...] = dot(to_rows, points[...].T, HIGH)


def scores(n_query, block, qb_ref, qaux_ref):
    keep = iota((block.shape[0], HALF), 1) < KEYED
    high = jnp.where(keep, block[:, HALF:], 0.0)
    first = high.astype(BF16).astype(F32)
    rest = high - first
    second = rest.astype(BF16).astype(F32)
    third = (rest - second).astype(BF16).astype(F32)
    split = first + pltpu.roll(second, KEYED, 1) + pltpu.roll(third, 2 * KEYED, 1)
    split = split.astype(BF16)
    row = iota((HALF, HALF), 0)
    lane = iota((HALF, HALF), 1)
    slot = lane % SLOTS
    heads = CHAIN // (3 * n_query)
    wanted = [
        jnp.where(slot < heads, n_query * (heads * a + slot) + p, -1)
        for a in range(3)
        for p in range(n_query)
    ]
    wanted += [jnp.full((HALF, HALF), CHAIN), jnp.full((HALF, HALF), PRESENT)]
    found = []
    for k in range(0, len(wanted), 2):
        picks = [
            ((row % KEYED == w) & (row < 3 * KEYED)).astype(F32).astype(BF16)
            for w in wanted[k : k + 2]
        ]
        both = dot(split, jnp.concatenate(picks, axis=1))
        found += [both[:, :HALF], both[:, HALF:]]
    used = 3 * n_query
    distance = jnp.zeros((block.shape[0], HALF), F32)
    for k in range(used):
        gap = qaux_ref[k : k + 1, :] - found[k]
        distance += gap * gap
    scale = qaux_ref[used : used + 1, :]
    bonus = qaux_ref[used + 1 : used + 2, :]
    differ = found[used] != qaux_ref[used + 2 : used + 3, :]
    there = found[used + 1] * qaux_ref[used + 3 : used + 4, :]
    partial = dot(block[:, :HALF], qb_ref[...], HIGH) + LOGIT_WEIGHT * (
        jnp.where(differ, bonus, 0.0) - scale * distance
    )
    return partial, MASK_PENALTY * (1.0 - there)


def softmax_sums(logits, block, turned_w):
    by_row = logits.T
    top = jnp.max(by_row, axis=1, keepdims=True)
    weights = jnp.exp(by_row - top)
    turned_w[...] = weights
    return top, dot(weights, block, HIGH)


def ascending(ref):
    return jnp.concatenate([ref[k] for k in reversed(range(ref.shape[0]))], axis=0)


def side(pair_ref, i, parity):
    _, far, _, half, width = pair_ref.shape
    return pair_ref[i, :, parity].reshape(far * half, width)


def pair_sums(turned_w, pair_ref, parity, g):
    width = pair_ref.shape[4]
    rows = slice(2 * SLOTS * g, 2 * SLOTS * (g + 1))
    right = jnp.concatenate(
        [side(pair_ref, 2 * g, parity), side(pair_ref, 2 * g + 1, parity)], axis=1
    )
    both = dot(turned_w[rows, :].astype(BF16), right)
    upper = iota((2 * SLOTS, width), 0) < SLOTS
    return rows, jnp.where(upper, both[:, :width], both[:, width:])


def near_kernel(
    heads,
    n_query,
    pair_ref,
    wb_hbm,
    mine_ref,
    qb_ref,
    qaux_ref,
    part_ref,
    bias_ref,
    weights,
    turned_w,
    wb_ref,
    sem,
):
    queries, far, _, half, width = pair_ref.shape
    keys = far * half
    place = lax.axis_index("blk") % 2
    small = pltpu.make_async_copy(wb_hbm, wb_ref, sem)
    small.start()
    block = ascending(mine_ref)
    partial, penalty = scores(n_query, block, qb_ref, qaux_ref)
    lane = iota((width, HALF), 1)
    row = iota((HALF, width), 0)
    small.wait()
    wb = wb_ref[...].astype(F32)
    each = jnp.zeros((HALF, width), F32)
    for h in range(heads):
        each = jnp.where(row % SLOTS == h, wb[h : h + 1, :], each)
    each = each.T
    for i in range(queries):
        weights[i * width : (i + 1) * width, :] = jnp.where(
            lane // SLOTS == i, each, 0.0
        ).astype(BF16)

    def bias_of(parity):
        left = jnp.concatenate([side(pair_ref, i, parity) for i in range(queries)], axis=1)
        return dot(left, weights[...])

    logits = (partial + LOGIT_WEIGHT * bias_of(place)) - penalty
    top, sums = softmax_sums(logits, block, turned_w)
    part_ref[:, HALF:] = jnp.where(iota(sums.shape, 1) == HALF + TOP, top, sums)
    for g in range(queries // 2):
        rows, found = pair_sums(turned_w, pair_ref, place, g)
        part_ref[rows, 0:width] = found
    bias_ref[...] = bias_of(1 - place)


def across_kernel(
    n_query, part_in, across_ref, bias_ref, qb_ref, qaux_ref, pair_ref, part_ref, turned_w
):
    width = pair_ref.shape[4]
    place = lax.axis_index("blk") % 2
    block = ascending(across_ref)
    partial, penalty = scores(n_query, block, qb_ref, qaux_ref)
    logits = (partial + LOGIT_WEIGHT * bias_ref[...]) - penalty
    top, sums = softmax_sums(logits, block, turned_w)
    before = part_in[:, 2 * HALF + TOP : 2 * HALF + TOP + 1]
    best = jnp.maximum(before, top)
    old, new = jnp.exp(before - best), jnp.exp(top - best)
    merged = part_in[:, HALF:] * old + sums * new
    part_ref[:, HALF:] = jnp.where(iota(sums.shape, 1) == HALF + TOP, best, merged)
    for g in range(pair_ref.shape[0] // 2):
        rows, found = pair_sums(turned_w, pair_ref, 1 - place, g)
        part_ref[rows, 0:width] = part_in[rows, 0:width] * old[rows, :] + found * new[rows, :]


def merge_kernel(
    heads,
    size,
    n_value,
    mine_ref,
    theirs_ref,
    frows_ref,
    w_out_ref,
    _,
    out_ref,
    small,
    large,
):
    copies, rows, _ = out_ref.shape
    tops = [ref[:, 2 * HALF + TOP : 2 * HALF + TOP + 1] for ref in (mine_ref, theirs_ref)]
    sums = [ref[:, 2 * HALF + ONE : 2 * HALF + ONE + 1] for ref in (mine_ref, theirs_ref)]
    best = jnp.maximum(tops[0], tops[1])
    factors = [jnp.exp(top - best) for top in tops]
    total = factors[0] * sums[0] + factors[1] * sums[1]
    merged = (mine_ref[...] * factors[0] + theirs_ref[...] * factors[1]) / total
    slot = iota((HALF, 1), 0) % SLOTS

    def of_own_head(first, step, count):
        picked = jnp.zeros((HALF, count), F32)
        for h in range(heads):
            at = first + step * h
            picked = jnp.where(slot == h, merged[:, at : at + count], picked)
        return picked

    attended = of_own_head(HALF + size, 2 * size, size)
    moved = [
        of_own_head(2 * HALF + KEYED + heads * n_value * a, n_value, n_value)
        - frows_ref[:, 9 + a : 10 + a]
        for a in range(3)
    ]
    pointed = []
    for b in range(3):
        total_b = frows_ref[:, b : b + 1] * moved[0]
        for a in (1, 2):
            total_b += frows_ref[:, 3 * a + b : 3 * a + b + 1] * moved[a]
        pointed.append(total_b)
    norms = jnp.sqrt(
        pointed[0] * pointed[0] + pointed[1] * pointed[1] + pointed[2] * pointed[2] + 1.0
    )
    small[...] = jnp.zeros_like(small)
    small[:, 0:size] = attended
    for b in range(3):
        small[:, size + n_value * b : size + n_value * (b + 1)] = pointed[b]
    edge = size + 3 * n_value
    small[:, edge : edge + n_value] = norms
    source = iota((HALF, HALF), 0)
    target = iota((HALF, HALF), 1)
    inside = (source >= size) & (source < edge)
    goes = jnp.where(
        inside, size + 3 * ((source - size) % n_value) + (source - size) // n_value, source
    )
    order = (goes == target).astype(F32).astype(BF16)
    small[...] = dot(small[...].astype(BF16), order)
    large[...] = merged[:, :HALF]
    cut = edge + n_value
    update = jnp.zeros((rows, w_out_ref.shape[2]), F32)
    for h in range(heads):
        low = small[pl.ds(h, rows, stride=SLOTS), :].astype(BF16)
        update += dot(low[:, :cut], w_out_ref[h, 0:cut, :])
        wide = large[pl.ds(h, rows, stride=SLOTS), :].astype(BF16)
        update += dot(wide, w_out_ref[h, cut:, :])
    for k in range(copies):
        out_ref[k] = update


def finish_kernel(updates_ref, single_ref, gain_ref, wb_ref, out_ref, send_ref):
    copies, rows, channels = updates_ref.shape
    mixed = single_ref[...].astype(F32)
    update = updates_ref[0]
    for k in range(1, copies):
        update += updates_ref[k]
    mixed = mixed + update
    centre = jnp.mean(mixed, axis=1, keepdims=True)
    away = mixed - centre
    spread = jnp.mean(away * away, axis=1, keepdims=True)
    gain = gain_ref[...].reshape(1, channels)
    single_out = (away * lax.rsqrt(spread + 1e-05) * gain).astype(BF16)
    out_ref[...] = single_out
    motion = dot_nt(wb_ref[...], single_out)
    groups = HALF // rows
    repeat = (iota((rows, HALF), 1) % rows == iota((rows, HALF), 0)).astype(F32)
    wide = dot(jnp.concatenate([motion, motion[:2]], axis=0), repeat, HIGH)
    group = iota((1, HALF), 1) // rows
    pieces = []
    for v in range(wide.shape[0] // groups):
        piece = wide[groups * v : groups * v + 1, :]
        for s in range(1, groups):
            at = groups * v + s
            piece = jnp.where(group == s, wide[at : at + 1, :], piece)
        pieces.append(piece)
    line = jnp.concatenate(pieces, axis=1)
    send_ref[...] = jnp.broadcast_to(line, (send_ref.shape[0], line.shape[1])).reshape(
        send_ref.shape
    )


def frames_kernel(edge, mine_ref, across_ref, out_ref, order):
    far, half, _ = mine_ref.shape
    place = lax.axis_index("blk") % 2
    which = lax.axis_index("pair")
    for ref, parity in ((mine_ref, place), (across_ref, 1 - place)):
        x = ref[:, :, :HALF].reshape(far * half, HALF)
        own = pltpu.roll(x, HALF - edge, 1)
        other = pltpu.roll(x, HALF - edge - 12, 1)
        for k in range(far):
            base = (2 * (far - 1 - k) + parity) * 2 * half
            rows = slice(k * half, (k + 1) * half)
            order[pl.ds(pl.multiple_of(base + which * half, half), half), :] = own[rows, :]
            order[pl.ds(pl.multiple_of(base + (1 - which) * half, half), half), :] = other[rows, :]
    for q in range(4 * far * half // HALF):
        at = slice(HALF * q, HALF * (q + 1))
        out_ref[:, at] = order[at, :].T[0:12, :]


def spread_kernel(first, blocks_ref, frames_ref, single_ref, out_ref, single_out_ref, motion):
    single_out_ref[...] = single_ref[...]
    blocks, _, wide = blocks_ref.shape
    rows = frames_ref.shape[1] // blocks
    groups = HALF // rows
    x = blocks_ref[...].reshape(blocks, wide)
    s = iota((blocks, HALF), 0) % groups
    g = iota((blocks, HALF), 1) // rows
    for v in range(wide // HALF):
        tile = x[:, HALF * v : HALF * (v + 1)]
        z = tile
        for d in range(1, groups):
            right = pltpu.roll(tile, rows * d, 1)
            up = pltpu.roll(right, blocks - d, 0)
            down = pltpu.roll(right, groups - d, 0)
            z = jnp.where(g - s == d, up, z)
            z = jnp.where(g - s == d - groups, down, z)
        for q in range(blocks // groups):
            at = (HALF * q + rows * first) % (rows * blocks)
            motion[groups * v : groups * (v + 1), at : at + HALF] = z[
                groups * q : groups * (q + 1), :
            ]
    m = [motion[k : k + 1, :] for k in range(6)]
    qa = 1.0 / jnp.sqrt(1.0 + m[0] * m[0] + m[1] * m[1] + m[2] * m[2])
    qb, qc, qd = m[0] * qa, m[1] * qa, m[2] * qa
    spin = [
        [qa * qa + qb * qb - qc * qc - qd * qd, 2.0 * (qb * qc - qa * qd), 2.0 * (qb * qd + qa * qc)],
        [2.0 * (qb * qc + qa * qd), qa * qa - qb * qb + qc * qc - qd * qd, 2.0 * (qc * qd - qa * qb)],
        [2.0 * (qb * qd - qa * qc), 2.0 * (qc * qd + qa * qb), qa * qa - qb * qb - qc * qc + qd * qd],
    ]
    for a in range(3):
        r = [frames_ref[3 * a + b : 3 * a + b + 1, :] for b in range(3)]
        for c in range(3):
            line = r[0] * spin[0][c] + r[1] * spin[1][c] + r[2] * spin[2][c]
            out_ref[3 * a + c : 3 * a + c + 1, :] = line
        moved = r[0] * m[3] + r[1] * m[4] + r[2] * m[5]
        out_ref[9 + a : 10 + a, :] = frames_ref[9 + a : 10 + a, :] + moved


def in_hbm(x):
    return pltpu.with_memory_space_constraint(x, pltpu.HBM)


def call(kernel, outs, scratch=(), specs=None, n=0, room=4, cost=None, name=None):
    return pl.pallas_call(
        kernel,
        out_shape=outs,
        in_specs=specs or [VMEM] * n,
        out_specs=jax.tree.map(lambda _: VMEM, outs),
        scratch_shapes=list(scratch),
        cost_estimate=cost,
        compiler_params=pltpu.CompilerParams(vmem_limit_bytes=room * 1024 * 1024),
        name=name,
    )


def body(
    single,
    pair,
    frames,
    chain,
    mask,
    w_query,
    w_key_value,
    w_query_points,
    w_kv_points,
    w_pair_bias,
    head_weights,
    chain_bias,
    w_out,
    out_gain,
    w_backbone,
):
    rows, channels = single.shape
    blocks, half = pair.shape[1], pair.shape[2]
    width = pair.shape[3]
    heads = w_pair_bias.shape[1]
    size = w_query.shape[1] // heads
    n_query = w_query_points.shape[1] // (3 * heads)
    n_points = w_kv_points.shape[1] // (3 * heads)
    n_value = n_points - n_query
    keys = blocks * half
    shape = jax.ShapeDtypeStruct

    inputs = (single, frames, chain, mask, w_key_value.T, w_kv_points.T)
    payload = call(
        functools.partial(keys_kernel, heads, size, n_query, n_points),
        shape((half, 2 * HALF), F32),
        (
            pltpu.VMEM((3 * heads * n_points, rows), F32),
            pltpu.VMEM((HALF, rows), F32),
            pltpu.VMEM((rows, 2 * HALF), F32),
            pltpu.VMEM((HALF, rows), F32),
            *(pltpu.VMEM(x.shape, x.dtype) for x in inputs),
            pltpu.SemaphoreType.DMA((len(inputs),)),
        ),
        specs=[HBM] * len(inputs),
        cost=pl.CostEstimate(flops=10**10, bytes_accessed=4 * pair.size, transcendentals=0),
        name="keys",
    )(*(in_hbm(x) for x in inputs))
    ways = [list(range(k, blocks, 2))[::-1] for k in range(2)]
    gathered = lax.all_gather(payload, "blk", axis=0, axis_index_groups=ways, tiled=False)
    swap = [(k, k + 1 - 2 * (k % 2)) for k in range(blocks)]
    across = lax.ppermute(gathered, "blk", swap)
    qb, qaux, frows = call(
        functools.partial(queries_kernel, heads, size, n_query),
        (shape((HALF, HALF), F32), shape((16, HALF), F32), shape((HALF, HALF), F32)),
        (
            pltpu.VMEM((3 * heads * n_query, rows), F32),
            pltpu.VMEM((HALF, rows), F32),
            pltpu.VMEM((104, rows), F32),
        ),
        specs=[VMEM] * 6 + [SMEM] * 2,
        cost=pl.CostEstimate(flops=10**8, bytes_accessed=10**5, transcendentals=0),
        name="queries",
    )(single, frames, chain, mask, w_query.T, w_query_points.T, head_weights, chain_bias)
    halves = pair.reshape(rows, blocks // 2, 2, half, width)
    part, bias = call(
        functools.partial(near_kernel, heads, n_query),
        (shape((HALF, 3 * HALF), F32), shape((keys // 2, HALF), F32)),
        (
            pltpu.VMEM((rows * width, HALF), BF16),
            pltpu.VMEM((HALF, keys // 2), F32),
            pltpu.VMEM((heads, width), w_pair_bias.dtype),
            pltpu.SemaphoreType.DMA,
        ),
        specs=[VMEM, HBM, VMEM, VMEM, VMEM],
        room=16,
        cost=pl.CostEstimate(flops=10**9, bytes_accessed=2 * pair.size, transcendentals=0),
        name="near",
    )(halves, in_hbm(w_pair_bias.T), gathered, qb, qaux)
    part = call(
        functools.partial(across_kernel, n_query),
        shape((HALF, 3 * HALF), F32),
        (pltpu.VMEM((HALF, keys // 2), F32),),
        n=6,
        room=16,
        name="across",
    )(part, across, bias, qb, qaux, halves)
    other = lax.ppermute(part, "pair", [(0, 1), (1, 0)])
    all_frames = call(
        functools.partial(frames_kernel, 2 * heads * size),
        shape((12, blocks * rows), F32),
        (pltpu.VMEM((blocks * rows, HALF), F32),),
        n=2,
        cost=pl.CostEstimate(flops=10**8, bytes_accessed=10**6, transcendentals=0),
        name="frames",
    )(gathered, across)
    updates = call(
        functools.partial(merge_kernel, heads, size, n_value),
        shape((lax.axis_size("head"), rows, channels), F32),
        (pltpu.VMEM((HALF, HALF), F32), pltpu.VMEM((HALF, HALF), F32)),
        n=5,
        name="merge",
    )(part, other, frows, w_out, all_frames)
    sides = lax.axis_size("head")
    last_first = [(k + sides - 1) % sides for k in range(sides)]
    updates = lax.all_to_all(
        updates, "head", split_axis=0, concat_axis=0, axis_index_groups=[last_first], tiled=True
    )
    single_here, send = call(
        finish_kernel,
        (shape((rows, channels), BF16), shape((blocks, 1, 8 * rows), F32)),
        n=4,
        name="finish",
    )(updates, single, out_gain, w_backbone.T)
    middle_first = [(k + blocks // 2) % blocks for k in range(blocks)]
    received = lax.all_to_all(
        send, "blk", split_axis=0, concat_axis=0, axis_index_groups=[middle_first], tiled=True
    )
    frames_out, single_out = call(
        functools.partial(spread_kernel, middle_first[0]),
        (shape((12, blocks * rows), F32), shape((rows, channels), BF16)),
        (pltpu.VMEM((8, blocks * rows), F32),),
        n=3,
        name="spread",
    )(received, all_frames, single_here)
    return (single_out, frames_out)


def solution(mesh):
    split = ("groups", "blk")
    placed = (
        P(split, None),
        P(split, None, "pair", None),
        P(None, split),
        P(split),
        P(split),
        P(None, "head"),
        P(None, "head"),
        P(None, "head"),
        P(None, "head"),
        P(None, "head"),
        P("head"),
        P("head"),
        P("head", None, None),
        P(),
        P(),
    )
    return jax.shard_map(
        body,
        mesh=mesh,
        in_specs=placed,
        out_specs=(P(split, None), P(None, "groups")),
        check_vma=False,
    )
```

```python
import functools
import math

import jax
import jax.numpy as jnp
from jax import lax
from jax.experimental import pallas as pl
from jax.experimental.pallas import tpu as pltpu
from jax.sharding import PartitionSpec as P

HIGH = lax.Precision.HIGHEST
LOGIT_WEIGHT = math.sqrt(1.0 / 3.0)
MASK_PENALTY = 100000.0
F32 = jnp.float32
BF16 = jnp.bfloat16

SLOTS = 4
HALF = 128
KEYED = 40
CHAIN, PRESENT, ONE, TOP = 36, 37, 38, 39
VMEM = pl.BlockSpec(memory_space=pltpu.VMEM)
SMEM = pl.BlockSpec(memory_space=pltpu.SMEM)
HBM = pl.BlockSpec(memory_space=pltpu.HBM)


def iota(shape, dim):
    return lax.broadcasted_iota(jnp.int32, shape, dim)


def dot(a, b, precision=None):
    return jnp.dot(a, b, preferred_element_type=F32, precision=precision)


def dot_nt(a, b):
    return lax.dot_general(a, b, (((1,), (1,)), ((), ())), preferred_element_type=F32)


def rotated(frames_ref, parts):
    moved = []
    for a in range(3):
        total = frames_ref[3 * a : 3 * a + 1, :] * parts[0]
        for b in (1, 2):
            total += frames_ref[3 * a + b : 3 * a + b + 1, :] * parts[b]
        moved.append(total + frames_ref[9 + a : 10 + a, :])
    return moved


def keys_kernel(heads, size, n_query, n_points, *refs):
    sources, refs = refs[:6], refs[6:]
    payload_ref, turned, points, full, spare = refs[:5]
    local_refs, sem = refs[5:11], refs[11]
    copies = [
        pltpu.make_async_copy(source, target, sem.at[k])
        for k, (source, target) in enumerate(zip(sources, local_refs))
    ]
    for copy in copies:
        copy.start()
    single_ref, frames_ref, chain_ref, mask_ref, wkv_ref, wkp_ref = local_refs
    spare[...] = jnp.zeros_like(spare)
    points[...] = jnp.zeros_like(points)
    for copy in copies:
        copy.wait()
    rows = single_ref.shape[0]
    half = payload_ref.shape[0]
    n_value = n_points - n_query
    x = single_ref[...]
    turned[...] = dot_nt(wkp_ref[...], x)
    edge = 2 * heads * size
    values = frames_ref[...]
    spare[edge : edge + 12, :] = values
    spare[edge + 12 : edge + 24, :] = jnp.concatenate([values[:, half:], values[:, :half]], axis=1)
    full[:, :HALF] = spare[...].T
    full[:, 0:edge] = dot_nt(x, wkv_ref[...])
    count = heads * n_points
    local = [turned[pl.ds(b, count, stride=3), :] for b in range(3)]
    for a, value in enumerate(rotated(frames_ref, local)):
        for h in range(heads):
            at = heads * n_query * a + n_query * h
            points[at : at + n_query, :] = value[n_points * h : n_points * h + n_query, :]
            at = KEYED + heads * n_value * a + n_value * h
            points[at : at + n_value, :] = value[n_points * h + n_query : n_points * (h + 1), :]
    points[CHAIN : CHAIN + 1, :] = chain_ref[...].astype(F32).reshape(1, rows)
    points[PRESENT : PRESENT + 1, :] = mask_ref[...].astype(F32).reshape(1, rows)
    points[ONE : ONE + 1, :] = jnp.ones((1, rows), F32)
    full[:, HALF:] = points[...].T
    start = pl.multiple_of(lax.axis_index("pair") * half, half)
    payload_ref[...] = full[pl.ds(start, half), :]


def queries_kernel(
    heads,
    size,
    n_query,
    single_ref,
    frames_ref,
    chain_ref,
    mask_ref,
    wq_ref,
    wqp_ref,
    hw_ref,
    cb_ref,
    qb_ref,
    qaux_ref,
    frows_ref,
    turned,
    points,
    spread,
):
    rows = single_ref.shape[0]
    x = single_ref[...]
    turned[...] = dot_nt(wqp_ref[...], x)
    count = heads * n_query
    local = [turned[pl.ds(b, count, stride=3), :] for b in range(3)]
    spread[...] = jnp.zeros_like(spread)
    spread[0 : heads * size, :] = dot_nt(wq_ref[...], x)
    for a, value in enumerate(rotated(frames_ref, local)):
        spread[48 + 16 * a : 48 + 16 * a + count, :] = value
    spread[96:97, :] = chain_ref[...].astype(F32).reshape(1, rows)
    spread[97:98, :] = mask_ref[...].astype(F32).reshape(1, rows)
    to_slots = (iota((rows, HALF), 1) // SLOTS == iota((rows, HALF), 0)).astype(F32)
    wide = dot(spread[...], to_slots, HIGH)
    slot = iota((1, HALF), 1) % SLOTS
    qb_ref[...] = jnp.zeros_like(qb_ref)
    scale = LOGIT_WEIGHT / math.sqrt(size)
    for h in range(heads):
        block = wide[h * size : (h + 1) * size, :] * scale
        qb_ref[2 * size * h : 2 * size * h + size, :] = jnp.where(slot == h, block, 0.0)
    qaux_ref[...] = jnp.zeros_like(qaux_ref)
    for a in range(3):
        for p in range(n_query):
            line = jnp.zeros((1, HALF), F32)
            for h in range(heads):
                at = 48 + 16 * a + h * n_query + p
                line = jnp.where(slot == h, wide[at : at + 1, :], line)
            qaux_ref[n_query * a + p : n_query * a + p + 1, :] = line
    raw = jnp.zeros((1, HALF), F32)
    bonus = jnp.zeros((1, HALF), F32)
    for h in range(heads):
        raw = jnp.where(slot == h, hw_ref[h], raw)
        bonus = jnp.where(slot == h, cb_ref[h], bonus)
    soft = jnp.maximum(raw, 0.0) + jnp.log1p(jnp.exp(-jnp.abs(raw)))
    used = 3 * n_query
    qaux_ref[used : used + 1, :] = soft * (math.sqrt(2.0 / (9.0 * n_query)) / 2.0)
    qaux_ref[used + 1 : used + 2, :] = bonus
    qaux_ref[used + 2 : used + 3, :] = wide[96:97, :]
    qaux_ref[used + 3 : used + 4, :] = wide[97:98, :]
    points[...] = jnp.zeros_like(points)
    points[0:12, :] = frames_ref[...]
    to_rows = (iota((HALF, rows), 0) // SLOTS == iota((HALF, rows), 1)).astype(F32)
    frows_ref[...] = dot(to_rows, points[...].T, HIGH)


def scores(n_query, block, qb_ref, qaux_ref):
    keep = iota((block.shape[0], HALF), 1) < KEYED
    high = jnp.where(keep, block[:, HALF:], 0.0)
    first = high.astype(BF16).astype(F32)
    rest = high - first
    second = rest.astype(BF16).astype(F32)
    third = (rest - second).astype(BF16).astype(F32)
    split = first + pltpu.roll(second, KEYED, 1) + pltpu.roll(third, 2 * KEYED, 1)
    split = split.astype(BF16)
    row = iota((HALF, HALF), 0)
    lane = iota((HALF, HALF), 1)
    slot = lane % SLOTS
    heads = CHAIN // (3 * n_query)
    wanted = [
        jnp.where(slot < heads, n_query * (heads * a + slot) + p, -1)
        for a in range(3)
        for p in range(n_query)
    ]
    wanted += [jnp.full((HALF, HALF), CHAIN), jnp.full((HALF, HALF), PRESENT)]
    found = []
    for k in range(0, len(wanted), 2):
        picks = [
            ((row % KEYED == w) & (row < 3 * KEYED)).astype(F32).astype(BF16)
            for w in wanted[k : k + 2]
        ]
        both = dot(split, jnp.concatenate(picks, axis=1))
        found += [both[:, :HALF], both[:, HALF:]]
    used = 3 * n_query
    distance = jnp.zeros((block.shape[0], HALF), F32)
    for k in range(used):
        gap = qaux_ref[k : k + 1, :] - found[k]
        distance += gap * gap
    scale = qaux_ref[used : used + 1, :]
    bonus = qaux_ref[used + 1 : used + 2, :]
    differ = found[used] != qaux_ref[used + 2 : used + 3, :]
    there = found[used + 1] * qaux_ref[used + 3 : used + 4, :]
    partial = dot(block[:, :HALF], qb_ref[...], HIGH) + LOGIT_WEIGHT * (
        jnp.where(differ, bonus, 0.0) - scale * distance
    )
    return partial, MASK_PENALTY * (1.0 - there)


def softmax_sums(logits, block, turned_w):
    by_row = logits.T
    top = jnp.max(by_row, axis=1, keepdims=True)
    weights = jnp.exp(by_row - top)
    turned_w[...] = weights
    return top, dot(weights, block, HIGH)


def ascending(ref):
    return jnp.concatenate([ref[k] for k in reversed(range(ref.shape[0]))], axis=0)


def side(pair_ref, i, parity):
    _, far, _, half, width = pair_ref.shape
    return pair_ref[i, :, parity].reshape(far * half, width)


def pair_sums(turned_w, pair_ref, parity, g):
    width = pair_ref.shape[4]
    rows = slice(2 * SLOTS * g, 2 * SLOTS * (g + 1))
    right = jnp.concatenate(
        [side(pair_ref, 2 * g, parity), side(pair_ref, 2 * g + 1, parity)], axis=1
    )
    both = dot(turned_w[rows, :].astype(BF16), right)
    upper = iota((2 * SLOTS, width), 0) < SLOTS
    return rows, jnp.where(upper, both[:, :width], both[:, width:])


def near_kernel(
    heads,
    n_query,
    pair_ref,
    wb_hbm,
    mine_ref,
    qb_ref,
    qaux_ref,
    part_ref,
    bias_ref,
    weights,
    turned_w,
    wb_ref,
    sem,
):
    queries, far, _, half, width = pair_ref.shape
    keys = far * half
    place = lax.axis_index("blk") % 2
    small = pltpu.make_async_copy(wb_hbm, wb_ref, sem)
    small.start()
    block = ascending(mine_ref)
    partial, penalty = scores(n_query, block, qb_ref, qaux_ref)
    lane = iota((width, HALF), 1)
    row = iota((HALF, width), 0)
    small.wait()
    wb = wb_ref[...].astype(F32)
    each = jnp.zeros((HALF, width), F32)
    for h in range(heads):
        each = jnp.where(row % SLOTS == h, wb[h : h + 1, :], each)
    each = each.T
    for i in range(queries):
        weights[i * width : (i + 1) * width, :] = jnp.where(
            lane // SLOTS == i, each, 0.0
        ).astype(BF16)

    def bias_of(parity):
        left = jnp.concatenate([side(pair_ref, i, parity) for i in range(queries)], axis=1)
        return dot(left, weights[...])

    logits = (partial + LOGIT_WEIGHT * bias_of(place)) - penalty
    top, sums = softmax_sums(logits, block, turned_w)
    part_ref[:, HALF:] = jnp.where(iota(sums.shape, 1) == HALF + TOP, top, sums)
    for g in range(queries // 2):
        rows, found = pair_sums(turned_w, pair_ref, place, g)
        part_ref[rows, 0:width] = found
    bias_ref[...] = bias_of(1 - place)


def across_kernel(
    n_query, part_in, across_ref, bias_ref, qb_ref, qaux_ref, pair_ref, part_ref, turned_w
):
    width = pair_ref.shape[4]
    place = lax.axis_index("blk") % 2
    block = ascending(across_ref)
    partial, penalty = scores(n_query, block, qb_ref, qaux_ref)
    logits = (partial + LOGIT_WEIGHT * bias_ref[...]) - penalty
    top, sums = softmax_sums(logits, block, turned_w)
    before = part_in[:, 2 * HALF + TOP : 2 * HALF + TOP + 1]
    best = jnp.maximum(before, top)
    old, new = jnp.exp(before - best), jnp.exp(top - best)
    merged = part_in[:, HALF:] * old + sums * new
    part_ref[:, HALF:] = jnp.where(iota(sums.shape, 1) == HALF + TOP, best, merged)
    for g in range(pair_ref.shape[0] // 2):
        rows, found = pair_sums(turned_w, pair_ref, 1 - place, g)
        part_ref[rows, 0:width] = part_in[rows, 0:width] * old[rows, :] + found * new[rows, :]


def merge_kernel(
    heads,
    size,
    n_value,
    mine_ref,
    theirs_ref,
    frows_ref,
    w_out_ref,
    _,
    out_ref,
    small,
    large,
):
    copies, rows, _ = out_ref.shape
    tops = [ref[:, 2 * HALF + TOP : 2 * HALF + TOP + 1] for ref in (mine_ref, theirs_ref)]
    sums = [ref[:, 2 * HALF + ONE : 2 * HALF + ONE + 1] for ref in (mine_ref, theirs_ref)]
    best = jnp.maximum(tops[0], tops[1])
    factors = [jnp.exp(top - best) for top in tops]
    total = factors[0] * sums[0] + factors[1] * sums[1]
    merged = (mine_ref[...] * factors[0] + theirs_ref[...] * factors[1]) / total
    slot = iota((HALF, 1), 0) % SLOTS

    def of_own_head(first, step, count):
        picked = jnp.zeros((HALF, count), F32)
        for h in range(heads):
            at = first + step * h
            picked = jnp.where(slot == h, merged[:, at : at + count], picked)
        return picked

    attended = of_own_head(HALF + size, 2 * size, size)
    moved = [
        of_own_head(2 * HALF + KEYED + heads * n_value * a, n_value, n_value)
        - frows_ref[:, 9 + a : 10 + a]
        for a in range(3)
    ]
    pointed = []
    for b in range(3):
        total_b = frows_ref[:, b : b + 1] * moved[0]
        for a in (1, 2):
            total_b += frows_ref[:, 3 * a + b : 3 * a + b + 1] * moved[a]
        pointed.append(total_b)
    norms = jnp.sqrt(
        pointed[0] * pointed[0] + pointed[1] * pointed[1] + pointed[2] * pointed[2] + 1.0
    )
    small[...] = jnp.zeros_like(small)
    small[:, 0:size] = attended
    for b in range(3):
        small[:, size + n_value * b : size + n_value * (b + 1)] = pointed[b]
    edge = size + 3 * n_value
    small[:, edge : edge + n_value] = norms
    source = iota((HALF, HALF), 0)
    target = iota((HALF, HALF), 1)
    inside = (source >= size) & (source < edge)
    goes = jnp.where(
        inside, size + 3 * ((source - size) % n_value) + (source - size) // n_value, source
    )
    order = (goes == target).astype(F32).astype(BF16)
    small[...] = dot(small[...].astype(BF16), order)
    large[...] = merged[:, :HALF]
    cut = edge + n_value
    update = jnp.zeros((rows, w_out_ref.shape[2]), F32)
    for h in range(heads):
        low = small[pl.ds(h, rows, stride=SLOTS), :].astype(BF16)
        update += dot(low[:, :cut], w_out_ref[h, 0:cut, :])
        wide = large[pl.ds(h, rows, stride=SLOTS), :].astype(BF16)
        update += dot(wide, w_out_ref[h, cut:, :])
    for k in range(copies):
        out_ref[k] = update


def finish_kernel(updates_ref, single_ref, gain_ref, wb_ref, out_ref, send_ref):
    copies, rows, channels = updates_ref.shape
    mixed = single_ref[...].astype(F32)
    update = updates_ref[0]
    for k in range(1, copies):
        update += updates_ref[k]
    mixed = mixed + update
    centre = jnp.mean(mixed, axis=1, keepdims=True)
    away = mixed - centre
    spread = jnp.mean(away * away, axis=1, keepdims=True)
    gain = gain_ref[...].reshape(1, channels)
    single_out = (away * lax.rsqrt(spread + 1e-05) * gain).astype(BF16)
    out_ref[...] = single_out
    motion = dot_nt(wb_ref[...], single_out)
    groups = HALF // rows
    repeat = (iota((rows, HALF), 1) % rows == iota((rows, HALF), 0)).astype(F32)
    wide = dot(jnp.concatenate([motion, motion[:2]], axis=0), repeat, HIGH)
    group = iota((1, HALF), 1) // rows
    pieces = []
    for v in range(wide.shape[0] // groups):
        piece = wide[groups * v : groups * v + 1, :]
        for s in range(1, groups):
            at = groups * v + s
            piece = jnp.where(group == s, wide[at : at + 1, :], piece)
        pieces.append(piece)
    line = jnp.concatenate(pieces, axis=1)
    send_ref[...] = jnp.broadcast_to(line, (send_ref.shape[0], line.shape[1])).reshape(
        send_ref.shape
    )


def frames_kernel(edge, mine_ref, across_ref, out_ref, order):
    far, half, _ = mine_ref.shape
    place = lax.axis_index("blk") % 2
    which = lax.axis_index("pair")
    for ref, parity in ((mine_ref, place), (across_ref, 1 - place)):
        x = ref[:, :, :HALF].reshape(far * half, HALF)
        own = pltpu.roll(x, HALF - edge, 1)
        other = pltpu.roll(x, HALF - edge - 12, 1)
        for k in range(far):
            base = (2 * (far - 1 - k) + parity) * 2 * half
            rows = slice(k * half, (k + 1) * half)
            order[pl.ds(pl.multiple_of(base + which * half, half), half), :] = own[rows, :]
            order[pl.ds(pl.multiple_of(base + (1 - which) * half, half), half), :] = other[rows, :]
    for q in range(4 * far * half // HALF):
        at = slice(HALF * q, HALF * (q + 1))
        out_ref[:, at] = order[at, :].T[0:12, :]


def spread_kernel(quads, blocks_ref, frames_ref, single_ref, out_ref, single_out_ref, motion):
    single_out_ref[...] = single_ref[...]
    blocks, _, wide = blocks_ref.shape
    rows = frames_ref.shape[1] // blocks
    groups = HALF // rows
    x = blocks_ref[...].reshape(blocks, wide)
    s = iota((blocks, HALF), 0) % groups
    g = iota((blocks, HALF), 1) // rows
    for v in range(wide // HALF):
        tile = x[:, HALF * v : HALF * (v + 1)]
        z = tile
        for d in range(1, groups):
            right = pltpu.roll(tile, rows * d, 1)
            up = pltpu.roll(right, blocks - d, 0)
            down = pltpu.roll(right, groups - d, 0)
            z = jnp.where(g - s == d, up, z)
            z = jnp.where(g - s == d - groups, down, z)
        for q in range(blocks // groups):
            at = HALF * quads[q]
            motion[groups * v : groups * (v + 1), at : at + HALF] = z[
                groups * q : groups * (q + 1), :
            ]
    m = [motion[k : k + 1, :] for k in range(6)]
    qa = 1.0 / jnp.sqrt(1.0 + m[0] * m[0] + m[1] * m[1] + m[2] * m[2])
    qb, qc, qd = m[0] * qa, m[1] * qa, m[2] * qa
    spin = [
        [qa * qa + qb * qb - qc * qc - qd * qd, 2.0 * (qb * qc - qa * qd), 2.0 * (qb * qd + qa * qc)],
        [2.0 * (qb * qc + qa * qd), qa * qa - qb * qb + qc * qc - qd * qd, 2.0 * (qc * qd - qa * qb)],
        [2.0 * (qb * qd - qa * qc), 2.0 * (qc * qd + qa * qb), qa * qa - qb * qb - qc * qc + qd * qd],
    ]
    for a in range(3):
        r = [frames_ref[3 * a + b : 3 * a + b + 1, :] for b in range(3)]
        for c in range(3):
            line = r[0] * spin[0][c] + r[1] * spin[1][c] + r[2] * spin[2][c]
            out_ref[3 * a + c : 3 * a + c + 1, :] = line
        moved = r[0] * m[3] + r[1] * m[4] + r[2] * m[5]
        out_ref[9 + a : 10 + a, :] = frames_ref[9 + a : 10 + a, :] + moved


def in_hbm(x):
    return pltpu.with_memory_space_constraint(x, pltpu.HBM)


def call(kernel, outs, scratch=(), specs=None, n=0, room=4, cost=None, name=None):
    return pl.pallas_call(
        kernel,
        out_shape=outs,
        in_specs=specs or [VMEM] * n,
        out_specs=jax.tree.map(lambda _: VMEM, outs),
        scratch_shapes=list(scratch),
        cost_estimate=cost,
        compiler_params=pltpu.CompilerParams(vmem_limit_bytes=room * 1024 * 1024),
        name=name,
    )


def body(
    single,
    pair,
    frames,
    chain,
    mask,
    w_query,
    w_key_value,
    w_query_points,
    w_kv_points,
    w_pair_bias,
    head_weights,
    chain_bias,
    w_out,
    out_gain,
    w_backbone,
):
    rows, channels = single.shape
    blocks, half = pair.shape[1], pair.shape[2]
    width = pair.shape[3]
    heads = w_pair_bias.shape[1]
    size = w_query.shape[1] // heads
    n_query = w_query_points.shape[1] // (3 * heads)
    n_points = w_kv_points.shape[1] // (3 * heads)
    n_value = n_points - n_query
    keys = blocks * half
    shape = jax.ShapeDtypeStruct

    inputs = (single, frames, chain, mask, w_key_value.T, w_kv_points.T)
    payload = call(
        functools.partial(keys_kernel, heads, size, n_query, n_points),
        shape((half, 2 * HALF), F32),
        (
            pltpu.VMEM((3 * heads * n_points, rows), F32),
            pltpu.VMEM((HALF, rows), F32),
            pltpu.VMEM((rows, 2 * HALF), F32),
            pltpu.VMEM((HALF, rows), F32),
            *(pltpu.VMEM(x.shape, x.dtype) for x in inputs),
            pltpu.SemaphoreType.DMA((len(inputs),)),
        ),
        specs=[HBM] * len(inputs),
        cost=pl.CostEstimate(flops=10**10, bytes_accessed=4 * pair.size, transcendentals=0),
        name="keys",
    )(*(in_hbm(x) for x in inputs))
    ways = [list(range(k, blocks, 2))[::-1] for k in range(2)]
    gathered = lax.all_gather(payload, "blk", axis=0, axis_index_groups=ways, tiled=False)
    swap = [(k, k + 1 - 2 * (k % 2)) for k in range(blocks)]
    across = lax.ppermute(gathered, "blk", swap)
    qb, qaux, frows = call(
        functools.partial(queries_kernel, heads, size, n_query),
        (shape((HALF, HALF), F32), shape((16, HALF), F32), shape((HALF, HALF), F32)),
        (
            pltpu.VMEM((3 * heads * n_query, rows), F32),
            pltpu.VMEM((HALF, rows), F32),
            pltpu.VMEM((104, rows), F32),
        ),
        specs=[VMEM] * 6 + [SMEM] * 2,
        cost=pl.CostEstimate(flops=10**8, bytes_accessed=10**5, transcendentals=0),
        name="queries",
    )(single, frames, chain, mask, w_query.T, w_query_points.T, head_weights, chain_bias)
    halves = pair.reshape(rows, blocks // 2, 2, half, width)
    part, bias = call(
        functools.partial(near_kernel, heads, n_query),
        (shape((HALF, 3 * HALF), F32), shape((keys // 2, HALF), F32)),
        (
            pltpu.VMEM((rows * width, HALF), BF16),
            pltpu.VMEM((HALF, keys // 2), F32),
            pltpu.VMEM((heads, width), w_pair_bias.dtype),
            pltpu.SemaphoreType.DMA,
        ),
        specs=[VMEM, HBM, VMEM, VMEM, VMEM],
        room=16,
        cost=pl.CostEstimate(flops=10**9, bytes_accessed=2 * pair.size, transcendentals=0),
        name="near",
    )(halves, in_hbm(w_pair_bias.T), gathered, qb, qaux)
    part = call(
        functools.partial(across_kernel, n_query),
        shape((HALF, 3 * HALF), F32),
        (pltpu.VMEM((HALF, keys // 2), F32),),
        n=6,
        room=16,
        name="across",
    )(part, across, bias, qb, qaux, halves)
    other = lax.ppermute(part, "pair", [(0, 1), (1, 0)])
    all_frames = call(
        functools.partial(frames_kernel, 2 * heads * size),
        shape((12, blocks * rows), F32),
        (pltpu.VMEM((blocks * rows, HALF), F32),),
        n=2,
        cost=pl.CostEstimate(flops=10**8, bytes_accessed=10**6, transcendentals=0),
        name="frames",
    )(gathered, across)
    updates = call(
        functools.partial(merge_kernel, heads, size, n_value),
        shape((lax.axis_size("head"), rows, channels), F32),
        (pltpu.VMEM((HALF, HALF), F32), pltpu.VMEM((HALF, HALF), F32)),
        n=5,
        name="merge",
    )(part, other, frows, w_out, all_frames)
    sides = lax.axis_size("head")
    last_first = [(k + sides - 1) % sides for k in range(sides)]
    updates = lax.all_to_all(
        updates, "head", split_axis=0, concat_axis=0, axis_index_groups=[last_first], tiled=True
    )
    single_here, send = call(
        finish_kernel,
        (shape((rows, channels), BF16), shape((blocks, 1, 8 * rows), F32)),
        n=4,
        name="finish",
    )(updates, single, out_gain, w_backbone.T)
    per = HALF // rows
    count = blocks // per
    outward = [(count + k // 2 if k % 2 == 0 else count - 1 - k // 2) % count for k in range(count)]
    quads = [count // 2] + [q for q in outward if q != count // 2]
    order = [per * q + k for q in quads for k in range(per)]
    received = lax.all_to_all(
        send, "blk", split_axis=0, concat_axis=0, axis_index_groups=[order], tiled=True
    )
    frames_out, single_out = call(
        functools.partial(spread_kernel, quads),
        (shape((12, blocks * rows), F32), shape((rows, channels), BF16)),
        (pltpu.VMEM((8, blocks * rows), F32),),
        n=3,
        name="spread",
    )(received, all_frames, single_here)
    return (single_out, frames_out)


def solution(mesh):
    split = ("groups", "blk")
    placed = (
        P(split, None),
        P(split, None, "pair", None),
        P(None, split),
        P(split),
        P(split),
        P(None, "head"),
        P(None, "head"),
        P(None, "head"),
        P(None, "head"),
        P(None, "head"),
        P("head"),
        P("head"),
        P("head", None, None),
        P(),
        P(),
    )
    return jax.shard_map(
        body,
        mesh=mesh,
        in_specs=placed,
        out_specs=(P(split, None), P(None, "groups")),
        check_vma=False,
    )
```
